16 devices in a mesh: data: 16 (over z, y, x, core).
Axes of the slice: x: 2, y: 2, z: 2, core: 2. Of those that a mesh axis runs over, the one named last changes fastest.
Arguments:
- feat_img: bfloat16 [16384, 768], P('data')
- feat_txt: bfloat16 [16384, 768], P('data')
- w_img: bfloat16 [768, 768], replicated
- w_txt: bfloat16 [768, 768], replicated
- log_temp: float32 [], replicated
- logit_bias: float32 [], replicated
- pair_ids: int32 [16384], P('data')
Outputs:
- output 1: float32 [], replicated
- output 2: float32 [], replicated
- output 3: float32 [], replicated
- output 4: float32 [768, 768], replicated
- output 5: float32 [768, 768], replicated
All inputs are finite; a program needn't handle non-finite values.
Results may differ from the reference program's by a relative error of at most 0.001.
Values are sent between devices in bfloat16 or wider.
A program may use at most 1 GiB of HBM per device.

```python
import jax
import jax.numpy as jnp
from jax import lax

ROWS_DEV = 1024
DEVICES = 16
EMBED = 768
FEAT_IMG = 768
FEAT_TXT = 768
LATENT = 16

BATCH = ROWS_DEV * DEVICES


def feature_draw(base_key, feat_width):
    key_list = jax.random.split(base_key, 4)
    latents = jax.random.normal(key_list[0], (BATCH, LATENT), jnp.float32)
    basis_rows = jax.random.normal(key_list[1], (LATENT, feat_width), jnp.float32)
    center = jax.random.normal(key_list[2], (feat_width,), jnp.float32)
    noise_rows = jax.random.normal(key_list[3], (BATCH, feat_width), jnp.float32)
    feat_out = center + jnp.dot(latents, basis_rows) * LATENT ** -0.5 + 0.5 * noise_rows
    return feat_out.astype(jnp.bfloat16)


def setup_inputs(seed: int = 0) -> dict:
    key_list = jax.random.split(jax.random.key(seed), 7)
    w_img = jax.random.normal(key_list[2], (FEAT_IMG, EMBED), jnp.float32) * FEAT_IMG ** -0.5
    w_txt = jax.random.normal(key_list[3], (FEAT_TXT, EMBED), jnp.float32) * FEAT_TXT ** -0.5
    log_temp = jnp.log(10.0) + jax.random.uniform(key_list[4], (), jnp.float32, -0.5, 0.5)
    logit_bias = -jnp.log(float(BATCH)) + jax.random.uniform(key_list[5], (), jnp.float32, -0.5, 1.5)
    pair_ids = (jax.random.permutation(key_list[6], BATCH) // 2).astype(jnp.int32)
    return {
        "feat_img": feature_draw(key_list[0], FEAT_IMG),
        "feat_txt": feature_draw(key_list[1], FEAT_TXT),
        "w_img": w_img.astype(jnp.bfloat16),
        "w_txt": w_txt.astype(jnp.bfloat16),
        "log_temp": log_temp.astype(jnp.float32),
        "logit_bias": logit_bias.astype(jnp.float32),
        "pair_ids": pair_ids,
    }


def reference(feat_img, feat_txt, w_img, w_txt, log_temp, logit_bias, pair_ids):
    temp_scale = jnp.exp(log_temp)
    raw_img = jnp.dot(feat_img, w_img, preferred_element_type=jnp.float32)
    raw_txt = jnp.dot(feat_txt, w_txt, preferred_element_type=jnp.float32)
    inv_img = lax.rsqrt(jnp.sum(raw_img * raw_img, axis=1, keepdims=True))
    inv_txt = lax.rsqrt(jnp.sum(raw_txt * raw_txt, axis=1, keepdims=True))
    unit_img = raw_img * inv_img
    unit_txt = raw_txt * inv_txt
    emb_img = unit_img.astype(jnp.bfloat16)
    emb_txt = unit_txt.astype(jnp.bfloat16)

    def row_block(loop_state, block_in):
        acc_txt, loss_sum, temp_sum, bias_sum = loop_state
        emb_blk, ids_blk = block_in
        sim_tile = jnp.dot(emb_blk, emb_txt.T, preferred_element_type=jnp.float32)
        label_sign = jnp.where(ids_blk[:, None] == pair_ids[None, :], 1.0, -1.0).astype(jnp.float32)
        margin = -label_sign * (temp_scale * sim_tile + logit_bias)
        grad_tile = -label_sign * jax.nn.sigmoid(margin) / BATCH
        grad_bf = grad_tile.astype(jnp.bfloat16)
        grad_blk = jnp.dot(grad_bf, emb_txt, preferred_element_type=jnp.float32)
        acc_txt = acc_txt + jnp.dot(grad_bf.T, emb_blk, preferred_element_type=jnp.float32)
        new_state = (
            acc_txt,
            loss_sum + jnp.sum(jax.nn.softplus(margin)),
            temp_sum + jnp.sum(grad_tile * sim_tile),
            bias_sum + jnp.sum(grad_tile),
        )
        return new_state, grad_blk

    zero_sum = jnp.zeros((), jnp.float32)
    init_state = (jnp.zeros((BATCH, EMBED), jnp.float32), zero_sum, zero_sum, zero_sum)
    block_in = (emb_img.reshape(DEVICES, ROWS_DEV, EMBED), pair_ids.reshape(DEVICES, ROWS_DEV))
    final_state, grad_blocks = lax.scan(row_block, init_state, block_in)
    acc_txt, loss_sum, temp_sum, bias_sum = final_state
    grad_img = temp_scale * grad_blocks.reshape(BATCH, EMBED)
    grad_txt = temp_scale * acc_txt
    raw_grad_img = inv_img * (grad_img - unit_img * jnp.sum(unit_img * grad_img, axis=1, keepdims=True))
    raw_grad_txt = inv_txt * (grad_txt - unit_txt * jnp.sum(unit_txt * grad_txt, axis=1, keepdims=True))
    grad_w_img = jnp.dot(feat_img.T, raw_grad_img.astype(jnp.bfloat16), preferred_element_type=jnp.float32)
    grad_w_txt = jnp.dot(feat_txt.T, raw_grad_txt.astype(jnp.bfloat16), preferred_element_type=jnp.float32)
    return loss_sum / BATCH, temp_scale * temp_sum, bias_sum, grad_w_img, grad_w_txt
```

```python
import jax
import jax.numpy as jnp
from jax import lax
from jax.experimental import pallas as pl
from jax.experimental.pallas import tpu as pltpu
from jax.sharding import PartitionSpec as P

F32, BF16 = jnp.float32, jnp.bfloat16
MESH = pl.DeviceIdType.MESH
ROWS, EMBED = 1024, 768
TILE_M, CHUNK_R = 512, 16
LOG2E = 1.4426950408889634
CONTRACT_ROWS = (((0,), (0,)), ((), ()))
CONTRACT_COLS = (((1,), (1,)), ((), ()))

SLOT = {0: 0, 1: 2, 2: 3, 4: 4, 3: 5, 6: 6, 5: 7, 7: 8}
PART_ROWS = ((0, 352), (352, 336), (688, 336))
PART_DIMS = ((1, 2, 4), (2, 4, 1), (4, 1, 2))


def embed_rows(feat_rows, weights):
    raw_emb = jnp.dot(feat_rows, weights, preferred_element_type=F32)
    inv_norm = lax.rsqrt(jnp.sum(raw_emb * raw_emb, axis=1, keepdims=True))
    unit_emb = raw_emb * inv_norm
    return unit_emb, inv_norm, unit_emb.astype(BF16)


def weight_grad(feat_rows, unit_emb, inv_norm, grad_emb):
    raw_grad = inv_norm * (grad_emb - unit_emb * jnp.sum(unit_emb * grad_emb, axis=1, keepdims=True))
    return lax.dot_general(feat_rows, raw_grad.astype(BF16), CONTRACT_ROWS, preferred_element_type=F32)


def gather_plan():
    own = [(p, 0, PART_DIMS[p][k]) for k in range(3) for p in range(3)]
    first, last = [], []
    for p, (d1, d2, d3) in enumerate(PART_DIMS):
        first.append((p, d1, d2))
    for p, (d1, d2, d3) in enumerate(PART_DIMS):
        first.append((p, d1, d3))
    for p, (d1, d2, d3) in enumerate(PART_DIMS):
        first.append((p, d2, d3))
    for p, (d1, d2, d3) in enumerate(PART_DIMS):
        last.append((p, d1 | d2, d3))
    return own, first, last


def pair_kernel(scal_ref, img_ref, txt_ref, ids_ref, idrow_ref, dimg_ref, dtxt_ref, sums_ref,
                slots, ids_all, id_rows, acc, partner, s0, s1, g0, g1, sums,
                send_sem, recv_sem, ids_send, ids_recv, pair_send, pair_recv, grad_send, grad_recv, load_sem):
    me = lax.axis_index("data")
    core = me % 2
    chip = me // 2

    def peer(rel):
        where = chip
        for d in (1, 2, 4):
            if rel & d:
                where = where + d * (1 - 2 * ((chip // d) % 2))
        return where * 2 + core

    other_core = chip * 2 + (1 - core)
    loads = [pltpu.make_async_copy(src, slots.at[a, 0], load_sem.at[a]) for a, src in ((0, txt_ref), (1, img_ref))]
    for c in loads:
        c.start()
    id_load = pltpu.make_async_copy(ids_ref, ids_all.at[0], load_sem.at[2])
    id_load.start()
    loads.append(pltpu.make_async_copy(idrow_ref, id_rows.at[pl.ds(0, ROWS)], load_sem.at[3]))
    loads[2].start()

    barrier = pltpu.get_barrier_semaphore()
    partners = [other_core] + [peer(rel) for rel in range(1, 8)]
    for dev in partners:
        pl.semaphore_signal(barrier, inc=1, device_id=(dev,), device_id_type=MESH)
    acc[...] = jnp.zeros_like(acc)
    sums[...] = jnp.zeros_like(sums)
    pl.semaphore_wait(barrier, len(partners))

    def part_copy(a, p, rel, d):
        lo, size = PART_ROWS[p]
        return pltpu.make_async_remote_copy(
            src_ref=slots.at[a, SLOT[rel], pl.ds(lo, size)],
            dst_ref=slots.at[a, SLOT[rel ^ d], pl.ds(lo, size)],
            send_sem=send_sem.at[a, p, SLOT[rel ^ d]],
            recv_sem=recv_sem.at[a, p, SLOT[rel ^ d]],
            device_id=(peer(d),), device_id_type=MESH)

    def arrival(a, p, rel):
        d = next(x for x in reversed(PART_DIMS[p]) if rel & x)
        part_copy(a, p, rel ^ d, d).wait_recv()

    own, first, last = gather_plan()
    pair_copies = [pltpu.make_async_remote_copy(
        src_ref=slots.at[a, 0], dst_ref=slots.at[a, 1], send_sem=pair_send.at[a], recv_sem=pair_recv.at[a],
        device_id=(other_core,), device_id_type=MESH) for a in range(2)]
    pair_copies.append(pltpu.make_async_remote_copy(
        src_ref=id_rows.at[pl.ds(0, ROWS)], dst_ref=id_rows.at[pl.ds(ROWS, ROWS)], send_sem=pair_send.at[2],
        recv_sem=pair_recv.at[2], device_id=(other_core,), device_id_type=MESH))
    id_copies = []
    for i, dev in enumerate(partners):
        rel_slot = 1 if i == 0 else SLOT[i]
        id_copies.append(pltpu.make_async_remote_copy(
            src_ref=ids_all.at[0], dst_ref=ids_all.at[rel_slot], send_sem=ids_send.at[rel_slot],
            recv_sem=ids_recv.at[rel_slot], device_id=(dev,), device_id_type=MESH))
    id_load.wait()
    for c in id_copies:
        c.start()
    for c in loads:
        c.wait()
    for c in pair_copies[::-1]:
        c.start()
    for send in own:
        part_copy(0, *send).start()

    scale, bias = scal_ref[0], scal_ref[1]
    for c in id_copies:
        c.wait_recv()
    for c in pair_copies:
        c.wait_recv()

    n_m = 2 * ROWS // TILE_M

    def slot_of(block):
        return block + (block + 7) // 8

    def scores(a, t, s_ref):
        m, slot = pl.multiple_of((t % n_m) * TILE_M, TILE_M), slot_of(t // n_m)
        rows = slots[1 - a, (t % n_m) // (n_m // 2), pl.ds(pl.multiple_of((t % (n_m // 2)) * TILE_M, TILE_M), TILE_M), :]
        s_ref[...] = lax.dot_general(rows, slots[a, slot], CONTRACT_COLS, preferred_element_type=F32)

    def tile_grad(a, t, s_ref, g_ref):
        m, slot = pl.multiple_of((t % n_m) * TILE_M, TILE_M), slot_of(t // n_m)

        col_ids = ids_all[slot]

        def rows_step(i, carry):
            x0, x1 = carry
            top = pl.multiple_of(i * CHUNK_R, CHUNK_R)
            row_ids = jnp.concatenate([id_rows[pl.ds(pl.multiple_of(m + top, CHUNK_R), CHUNK_R), :]] * 8, axis=1)
            sim = s_ref[pl.ds(top, CHUNK_R), :]
            sign = jnp.where(row_ids == col_ids, -1.0, 1.0)
            margin = sign * (scale * sim + bias)
            e = jnp.exp2(jnp.abs(margin) * (-LOG2E))
            d = 1.0 + e
            r = 1.0 / d
            grad = sign * jnp.where(margin >= 0, r, e * r)
            g_ref[pl.ds(top, CHUNK_R), :] = grad.astype(BF16)
            if a == 0:
                return x0 + jnp.maximum(margin, 0.0), x1 * d + e
            return x0 + grad * sim, x1 + grad

        x1 = jnp.zeros((CHUNK_R, ROWS), F32) if a == 0 else sums[3]
        x0, x1 = lax.fori_loop(0, TILE_M // CHUNK_R, rows_step, (sums[2 * a], x1), unroll=True)
        sums[2 * a] = x0
        sums[2 * a + 1] = sums[1] + jnp.log1p(x1) if a == 0 else x1

    def row_grad(a, t, g_ref):
        m, slot = pl.multiple_of((t % n_m) * TILE_M, TILE_M), slot_of(t // n_m)
        acc[1 - a, pl.ds(m, TILE_M), :] += jnp.dot(g_ref[...], slots[a, slot], preferred_element_type=F32)

    def block_needs(a, rel, seen):
        return [(a, p, rel) for p in range(3) if (a, p, rel) not in seen]

    order = sorted(SLOT, key=SLOT.get)
    seen = set()
    steps = {}

    def add(key, waits=(), sends=()):
        w = [x for x in dict.fromkeys(waits) if x not in seen]
        seen.update(w)
        steps.setdefault(key, []).append((w, list(sends)))

    def forwards(a, sends):
        return [(a, p, rel) for p, rel, _ in sends], [(a,) + s for s in sends]

    add((0, 1), *forwards(0, first))
    add((0, 1), block_needs(0, order[1], seen))
    add((0, 2), block_needs(0, order[2], seen))
    add((0, 2), *forwards(0, last))
    add((0, 2), (), [(1,) + s for s in own])
    for b in range(3, 8):
        add((0, b), block_needs(0, order[b], seen))
    add((0, 7), *forwards(1, first))
    add((1, 1), block_needs(1, order[1], seen))
    add((1, 2), block_needs(1, order[2], seen))
    add((1, 2), *forwards(1, last))
    for b in range(3, 8):
        add((1, b), block_needs(1, order[b], seen))

    def run_steps(key):
        for waits, sends in steps.get(key, ()):
            for w in waits:
                arrival(*w)
            for s in sends:
                part_copy(*s).start()

    def stream(a):
        t0, t_end = 0, 8 * n_m
        scores(a, t0, s0)
        scores(a, t0 + 1, s1)
        tile_grad(a, t0, s0, g0)

        def body(k, carry):
            t = t0 + 2 * k + 1
            for b in range(1, 8):
                @pl.when(t + 1 == b * n_m)
                def _():
                    run_steps((a, b))
            scores(a, t + 1, s0)
            tile_grad(a, t, s1, g1)
            row_grad(a, t - 1, g0)
            scores(a, t + 2, s1)
            tile_grad(a, t + 1, s0, g0)
            row_grad(a, t, g1)
            return carry

        lax.fori_loop(0, (t_end - t0 - 2) // 2, body, 0)
        tile_grad(a, t_end - 1, s1, g1)
        row_grad(a, t_end - 2, g0)
        row_grad(a, t_end - 1, g1)

    grad_copies = [pltpu.make_async_remote_copy(
        src_ref=acc.at[x, pl.ds(ROWS, ROWS)], dst_ref=partner.at[x], send_sem=grad_send.at[x],
        recv_sem=grad_recv.at[x], device_id=(other_core,), device_id_type=MESH) for x in range(2)]

    stream(0)
    grad_copies[1].start()
    stream(1)
    grad_copies[0].start()
    grad_copies[1].wait_recv()
    acc[1, 0:ROWS, :] += partner[1]
    outs = [pltpu.make_async_copy(acc.at[x, pl.ds(0, ROWS)], ref, load_sem.at[x]) for x, ref in ((1, dimg_ref), (0, dtxt_ref))]
    outs[0].start()
    sums_ref[...] = sums[...]
    grad_copies[0].wait_recv()
    acc[0, 0:ROWS, :] += partner[0]
    outs[1].start()
    for c in outs:
        c.wait()
    for c in grad_copies + pair_copies + id_copies:
        c.wait_send()
    for a in range(2):
        for send in own + first + last:
            part_copy(a, *send).wait_send()


def solution(mesh):
    n_dev = mesh.shape["data"]

    def local_fn(feat_img, feat_txt, w_img, w_txt, log_temp, logit_bias, pair_ids):
        total_rows = feat_img.shape[0] * n_dev
        temp_scale = jnp.exp(log_temp)
        unit_img, inv_img, emb_img = embed_rows(feat_img, w_img)
        unit_txt, inv_txt, emb_txt = embed_rows(feat_txt, w_txt)
        vmem = pl.BlockSpec(memory_space=pltpu.VMEM)
        hbm = pl.BlockSpec(memory_space=pl.ANY)
        dma = pltpu.SemaphoreType.DMA
        part_img, part_txt, sums = pl.pallas_call(
            pair_kernel,
            out_shape=[jax.ShapeDtypeStruct((ROWS, EMBED), F32)] * 2 + [jax.ShapeDtypeStruct((4, CHUNK_R, ROWS), F32)],
            in_specs=[pl.BlockSpec(memory_space=pltpu.SMEM), hbm, hbm, hbm, hbm],
            out_specs=[hbm, hbm, vmem],
            scratch_shapes=[
                pltpu.VMEM((2, 9, ROWS, EMBED), BF16),
                pltpu.VMEM((9, 1, ROWS), jnp.int32),
                pltpu.VMEM((2 * ROWS, 128), jnp.int32),
                pltpu.VMEM((2, 2 * ROWS, EMBED), F32),
                pltpu.VMEM((2, ROWS, EMBED), F32),
                pltpu.VMEM((TILE_M, ROWS), F32), pltpu.VMEM((TILE_M, ROWS), F32),
                pltpu.VMEM((TILE_M, ROWS), BF16), pltpu.VMEM((TILE_M, ROWS), BF16),
                pltpu.VMEM((4, CHUNK_R, ROWS), F32),
                dma((2, 3, 9)), dma((2, 3, 9)), dma((9,)), dma((9,)), dma((3,)), dma((3,)), dma((2,)), dma((2,)),
                dma((4,)),
            ],
            compiler_params=pltpu.CompilerParams(
                collective_id=0, has_side_effects=True, vmem_limit_bytes=66_000_000),
            cost_estimate=pl.CostEstimate(flops=110_000_000_000, bytes_accessed=16_000_000, transcendentals=0),
        )(jnp.stack([temp_scale, logit_bias]), emb_img, emb_txt, pair_ids.reshape(1, ROWS),
          jnp.broadcast_to(pair_ids[:, None], (ROWS, 128)))
        grad_img = temp_scale * (part_img / total_rows)
        grad_txt = temp_scale * (part_txt / total_rows)
        dw_img = weight_grad(feat_img, unit_img, inv_img, grad_img)
        dw_txt = weight_grad(feat_txt, unit_txt, inv_txt, grad_txt)
        loss_sum = jnp.sum(sums[0]) + jnp.sum(sums[1])
        totals = lax.psum((loss_sum, jnp.sum(sums[2]), jnp.sum(sums[3]), dw_img, dw_txt), "data")
        return totals[0] / total_rows, temp_scale * (totals[1] / total_rows), totals[2] / total_rows, totals[3], totals[4]

    return jax.shard_map(
        local_fn,
        mesh=mesh,
        in_specs=(P("data", None), P("data", None), P(None, None), P(None, None), P(), P(), P("data")),
        out_specs=(P(), P(), P(), P(None, None), P(None, None)),
        check_vma=False,
    )
```

```python
import jax
import jax.numpy as jnp
from jax import lax
from jax.experimental import pallas as pl
from jax.experimental.pallas import tpu as pltpu
from jax.sharding import PartitionSpec as P

F32, BF16 = jnp.float32, jnp.bfloat16
MESH = pl.DeviceIdType.MESH
ROWS, EMBED = 1024, 768
TILE_M, CHUNK_R = 512, 16
LOG2E = 1.4426950408889634
CONTRACT_ROWS = (((0,), (0,)), ((), ()))
CONTRACT_COLS = (((1,), (1,)), ((), ()))

SLOT = {0: 0, 1: 2, 2: 3, 4: 4, 3: 5, 6: 6, 5: 7, 7: 8}
PART_ROWS = ((0, 352), (352, 336), (688, 336))
PART_DIMS = ((1, 2, 4), (2, 4, 1), (4, 1, 2))


def gather_plan():
    own = [(p, 0, PART_DIMS[p][k]) for k in range(3) for p in range(3)]
    first, last = [], []
    for p, (d1, d2, d3) in enumerate(PART_DIMS):
        first.append((p, d1, d2))
    for p, (d1, d2, d3) in enumerate(PART_DIMS):
        first.append((p, d1, d3))
    for p, (d1, d2, d3) in enumerate(PART_DIMS):
        first.append((p, d2, d3))
    for p, (d1, d2, d3) in enumerate(PART_DIMS):
        last.append((p, d1 | d2, d3))
    return own, first, last


def pair_kernel(scal_ref, feat_img, feat_txt, w_img, w_txt, ids_ref, idrow_ref, dimg_ref, dtxt_ref, sums_ref,
                slots, ids_all, id_rows, acc, partner, s0, s1, g0, g1, sums,
                send_sem, recv_sem, ids_send, ids_recv, pair_send, pair_recv, grad_send, grad_recv, load_sem):
    me = lax.axis_index("data")
    core = me % 2
    chip = me // 2

    def peer(rel):
        where = chip
        for d in (1, 2, 4):
            if rel & d:
                where = where + d * (1 - 2 * ((chip // d) % 2))
        return where * 2 + core

    other_core = chip * 2 + (1 - core)
    loads = [pltpu.make_async_copy(src, slots.at[a, 8], load_sem.at[2 * a]) for a, src in ((0, feat_txt), (1, feat_img))]
    loads += [pltpu.make_async_copy(src, slots.at[a, 7, pl.ds(0, EMBED)], load_sem.at[2 * a + 1])
              for a, src in ((0, w_txt), (1, w_img))]
    loads.append(pltpu.make_async_copy(ids_ref, ids_all.at[0], load_sem.at[4]))
    loads.append(pltpu.make_async_copy(idrow_ref, id_rows.at[pl.ds(0, ROWS)], load_sem.at[5]))
    for c in loads:
        c.start()
    acc[...] = jnp.zeros_like(acc)
    sums[...] = jnp.zeros_like(sums)
    for c in loads:
        c.wait()

    def embed(i, carry):
        a, rows = i // 2, pl.ds(pl.multiple_of((i % 2) * (ROWS // 2), ROWS // 2), ROWS // 2)
        raw = jnp.dot(slots[a, 8, rows, :], slots[a, 7, 0:EMBED, :], preferred_element_type=F32)
        slots[a, 0, rows, :] = (raw * lax.rsqrt(jnp.sum(raw * raw, axis=1, keepdims=True))).astype(BF16)
        return carry

    lax.fori_loop(0, 4, embed, 0)

    barrier = pltpu.get_barrier_semaphore()
    partners = [other_core] + [peer(rel) for rel in range(1, 8)]
    for dev in partners:
        pl.semaphore_signal(barrier, inc=1, device_id=(dev,), device_id_type=MESH)
    pl.semaphore_wait(barrier, len(partners))

    def part_copy(a, p, rel, d):
        lo, size = PART_ROWS[p]
        return pltpu.make_async_remote_copy(
            src_ref=slots.at[a, SLOT[rel], pl.ds(lo, size)],
            dst_ref=slots.at[a, SLOT[rel ^ d], pl.ds(lo, size)],
            send_sem=send_sem.at[a, p, SLOT[rel ^ d]],
            recv_sem=recv_sem.at[a, p, SLOT[rel ^ d]],
            device_id=(peer(d),), device_id_type=MESH)

    def arrival(a, p, rel):
        d = next(x for x in reversed(PART_DIMS[p]) if rel & x)
        part_copy(a, p, rel ^ d, d).wait_recv()

    own, first, last = gather_plan()
    pair_copies = [pltpu.make_async_remote_copy(
        src_ref=slots.at[a, 0], dst_ref=slots.at[a, 1], send_sem=pair_send.at[a], recv_sem=pair_recv.at[a],
        device_id=(other_core,), device_id_type=MESH) for a in range(2)]
    pair_copies.append(pltpu.make_async_remote_copy(
        src_ref=id_rows.at[pl.ds(0, ROWS)], dst_ref=id_rows.at[pl.ds(ROWS, ROWS)], send_sem=pair_send.at[2],
        recv_sem=pair_recv.at[2], device_id=(other_core,), device_id_type=MESH))
    id_copies = []
    for i, dev in enumerate(partners):
        rel_slot = 1 if i == 0 else SLOT[i]
        id_copies.append(pltpu.make_async_remote_copy(
            src_ref=ids_all.at[0], dst_ref=ids_all.at[rel_slot], send_sem=ids_send.at[rel_slot],
            recv_sem=ids_recv.at[rel_slot], device_id=(dev,), device_id_type=MESH))
    for c in id_copies:
        c.start()
    for c in pair_copies[::-1]:
        c.start()
    for send in own:
        part_copy(0, *send).start()

    scale, bias = scal_ref[0], scal_ref[1]
    for c in id_copies:
        c.wait_recv()
    for c in pair_copies:
        c.wait_recv()

    n_m = 2 * ROWS // TILE_M

    def slot_of(block):
        return block + (block + 7) // 8

    def scores(a, t, s_ref):
        m, slot = pl.multiple_of((t % n_m) * TILE_M, TILE_M), slot_of(t // n_m)
        rows = slots[1 - a, (t % n_m) // (n_m // 2), pl.ds(pl.multiple_of((t % (n_m // 2)) * TILE_M, TILE_M), TILE_M), :]
        s_ref[...] = lax.dot_general(rows, slots[a, slot], CONTRACT_COLS, preferred_element_type=F32)

    def tile_grad(a, t, s_ref, g_ref):
        m, slot = pl.multiple_of((t % n_m) * TILE_M, TILE_M), slot_of(t // n_m)

        col_ids = ids_all[slot]

        def rows_step(i, carry):
            x0, x1 = carry
            top = pl.multiple_of(i * CHUNK_R, CHUNK_R)
            row_ids = jnp.concatenate([id_rows[pl.ds(pl.multiple_of(m + top, CHUNK_R), CHUNK_R), :]] * 8, axis=1)
            sim = s_ref[pl.ds(top, CHUNK_R), :]
            sign = jnp.where(row_ids == col_ids, -1.0, 1.0)
            margin = sign * (scale * sim + bias)
            e = jnp.exp2(jnp.abs(margin) * (-LOG2E))
            d = 1.0 + e
            r = 1.0 / d
            grad = sign * jnp.where(margin >= 0, r, e * r)
            g_ref[pl.ds(top, CHUNK_R), :] = grad.astype(BF16)
            if a == 0:
                return x0 + jnp.maximum(margin, 0.0), x1 * d + e
            return x0 + grad * sim, x1 + grad

        x1 = jnp.zeros((CHUNK_R, ROWS), F32) if a == 0 else sums[3]
        x0, x1 = lax.fori_loop(0, TILE_M // CHUNK_R, rows_step, (sums[2 * a], x1), unroll=True)
        sums[2 * a] = x0
        sums[2 * a + 1] = sums[1] + jnp.log1p(x1) if a == 0 else x1

    def row_grad(a, t, g_ref):
        m, slot = pl.multiple_of((t % n_m) * TILE_M, TILE_M), slot_of(t // n_m)
        acc[1 - a, pl.ds(m, TILE_M), :] += jnp.dot(g_ref[...], slots[a, slot], preferred_element_type=F32)

    def block_needs(a, rel, seen):
        return [(a, p, rel) for p in range(3) if (a, p, rel) not in seen]

    order = sorted(SLOT, key=SLOT.get)
    seen = set()
    steps = {}

    def add(key, waits=(), sends=()):
        w = [x for x in dict.fromkeys(waits) if x not in seen]
        seen.update(w)
        steps.setdefault(key, []).append((w, list(sends)))

    def forwards(a, sends):
        return [(a, p, rel) for p, rel, _ in sends], [(a,) + s for s in sends]

    add((0, 1), *forwards(0, first))
    add((0, 1), block_needs(0, order[1], seen))
    add((0, 2), block_needs(0, order[2], seen))
    add((0, 2), *forwards(0, last))
    add((0, 2), (), [(1,) + s for s in own])
    for b in range(3, 8):
        add((0, b), block_needs(0, order[b], seen))
    add((0, 7), *forwards(1, first))
    add((1, 1), block_needs(1, order[1], seen))
    add((1, 2), block_needs(1, order[2], seen))
    add((1, 2), *forwards(1, last))
    for b in range(3, 8):
        add((1, b), block_needs(1, order[b], seen))

    def run_steps(key):
        for waits, sends in steps.get(key, ()):
            for w in waits:
                arrival(*w)
            for s in sends:
                part_copy(*s).start()

    def stream(a):
        t0, t_end = 0, 8 * n_m
        scores(a, t0, s0)
        scores(a, t0 + 1, s1)
        tile_grad(a, t0, s0, g0)

        def body(k, carry):
            t = t0 + 2 * k + 1
            for b in range(1, 8):
                @pl.when(t + 1 == b * n_m)
                def _():
                    run_steps((a, b))
            scores(a, t + 1, s0)
            tile_grad(a, t, s1, g1)
            row_grad(a, t - 1, g0)
            scores(a, t + 2, s1)
            tile_grad(a, t + 1, s0, g0)
            row_grad(a, t, g1)
            return carry

        lax.fori_loop(0, (t_end - t0 - 2) // 2, body, 0)
        tile_grad(a, t_end - 1, s1, g1)
        row_grad(a, t_end - 2, g0)
        row_grad(a, t_end - 1, g1)

    grad_copies = [pltpu.make_async_remote_copy(
        src_ref=acc.at[x, pl.ds(ROWS, ROWS)], dst_ref=partner.at[x], send_sem=grad_send.at[x],
        recv_sem=grad_recv.at[x], device_id=(other_core,), device_id_type=MESH) for x in range(2)]

    stream(0)
    grad_copies[1].start()
    stream(1)
    grad_copies[0].start()
    grad_copies[1].wait_recv()
    acc[1, 0:ROWS, :] += partner[1]
    outs = [pltpu.make_async_copy(acc.at[x, pl.ds(0, ROWS)], ref, load_sem.at[x]) for x, ref in ((1, dimg_ref), (0, dtxt_ref))]
    outs[0].start()
    for x in range(4):
        rows = sums[x, 0:8, :] + sums[x, 8:16, :]
        sums_ref[x] = sum(rows[:, v:v + 128] for v in range(0, ROWS, 128))
    grad_copies[0].wait_recv()
    acc[0, 0:ROWS, :] += partner[0]
    outs[1].start()
    for c in outs:
        c.wait()
    for c in grad_copies + pair_copies + id_copies:
        c.wait_send()
    for a in range(2):
        for send in own + first + last:
            part_copy(a, *send).wait_send()


def tail_kernel(scal_ref, feat_img, feat_txt, w_img, w_txt, part_img, part_txt, sums_ref, dw_img_ref, dw_txt_ref, tot_ref,
                feats, heads, parts, raw_grad, mine, full, from_core, landing, stats,
                load_sem, core_send, core_recv, rs_send, rs_recv, ag_send, ag_recv, out_send, out_recv, st_send, st_recv, ready):
    me = lax.axis_index("data")
    core, chip = me % 2, me // 2
    other_core = chip * 2 + (1 - core)
    near = {d: (chip + d * (1 - 2 * ((chip // d) % 2))) * 2 + core for d in (1, 2, 4)}
    others = [(me + k) % 16 for k in range(1, 16)]

    loads = []
    for a, refs in enumerate(((feat_img, w_img, part_img), (feat_txt, w_txt, part_txt))):
        loads += [pltpu.make_async_copy(src, dst.at[a], load_sem.at[a, k])
                  for k, (src, dst) in enumerate(zip(refs, (feats, heads, parts)))]
    for c in loads:
        c.start()
    barrier = pltpu.get_barrier_semaphore()
    for dev in others:
        pl.semaphore_signal(barrier, inc=1, device_id=(dev,), device_id_type=MESH)
    for c in loads:
        c.wait()
    scale = scal_ref[0]
    total_rows = 16 * ROWS

    def head_grad(a, dst):
        def rows_step(i, carry):
            rows = pl.ds(pl.multiple_of(i * 256, 256), 256)
            raw = jnp.dot(feats[a, rows, :], heads[a], preferred_element_type=F32)
            inv = lax.rsqrt(jnp.sum(raw * raw, axis=1, keepdims=True))
            unit = raw * inv
            grad = scale * (parts[a, rows, :] * F32(1.0 / total_rows))
            raw_grad[rows, :] = (inv * (grad - unit * jnp.sum(unit * grad, axis=1, keepdims=True))).astype(BF16)
            return carry

        lax.fori_loop(0, ROWS // 256, rows_step, 0)
        dst[...] = lax.dot_general(feats[a], raw_grad[...], CONTRACT_ROWS, preferred_element_type=F32)

    head_grad(1 - core, full.at[1 - core])
    pl.semaphore_wait(barrier, len(others))
    to_core = pltpu.make_async_remote_copy(
        src_ref=full.at[1 - core], dst_ref=from_core, send_sem=core_send, recv_sem=core_recv,
        device_id=(other_core,), device_id_type=MESH)
    to_core.start()
    stats[me] = sums_ref[...]
    stat_copies = [pltpu.make_async_remote_copy(
        src_ref=stats.at[me], dst_ref=stats.at[me], send_sem=st_send.at[k], recv_sem=st_recv.at[k],
        device_id=(dev,), device_id_type=MESH) for k, dev in enumerate(others)]
    for c in stat_copies:
        c.start()
    head_grad(core, mine)
    to_core.wait_recv()
    mine[...] += from_core[...]

    lows = [256 * p for p in range(3)]
    kept = []
    sent = []
    for k, half in enumerate((128, 64, 32)):
        base = (0, 128, 192)[k]
        copies = []
        for p in range(3):
            d = PART_DIMS[p][k]
            bit = (chip // d) % 2
            src = pl.multiple_of(lows[p] + (1 - bit) * half, 32)
            copies.append(pltpu.make_async_remote_copy(
                src_ref=mine.at[pl.ds(src, half)], dst_ref=landing.at[p, pl.ds(base, half)],
                send_sem=rs_send.at[k, p], recv_sem=rs_recv.at[k, p], device_id=(near[d],), device_id_type=MESH))
            copies[-1].start()
        kept.append(list(lows))
        for p in range(3):
            bit = (chip // PART_DIMS[p][k]) % 2
            lows[p] = lows[p] + bit * half
            copies[p].wait_recv()
            rows = pl.ds(pl.multiple_of(lows[p], 32), half)
            total = mine[rows, :] + landing[p, base:base + half, :]
            if k < 2:
                mine[rows, :] = total
            else:
                full[core, rows, :] = total
        sent += copies

    def share(low, size, p, k):
        rows = pl.ds(pl.multiple_of(low, 32), size)
        return pltpu.make_async_remote_copy(
            src_ref=full.at[core, rows], dst_ref=full.at[core, rows], send_sem=out_send.at[p, k],
            recv_sem=out_recv.at[p, k], device_id=(other_core,), device_id_type=MESH)

    to_core.wait_send()
    pl.semaphore_signal(ready, inc=1, device_id=(other_core,), device_id_type=MESH)
    pl.semaphore_wait(ready, 1)
    shares = []
    for k in (2, 1, 0):
        size = (128, 64, 32)[k]
        copies = []
        for p in range(3):
            d = PART_DIMS[p][k]
            rows = pl.ds(pl.multiple_of(lows[p], 32), size)
            copies.append(pltpu.make_async_remote_copy(
                src_ref=full.at[core, rows], dst_ref=full.at[core, rows], send_sem=ag_send.at[k, p],
                recv_sem=ag_recv.at[k, p], device_id=(near[d],), device_id_type=MESH))
            copies[-1].start()
        if k == 2:
            for p in range(3):
                shares.append(share(lows[p], size, p, 3))
                shares[-1].start()
        for p in range(3):
            bit = (chip // PART_DIMS[p][k]) % 2
            copies[p].wait_recv()
            shares.append(share(kept[k][p] + (1 - bit) * size, size, p, k))
            shares[-1].start()
            lows[p] = kept[k][p]
        sent += copies
    write_mine = [pltpu.make_async_copy(full.at[a], ref, load_sem.at[a, 0]) for a, ref in ((0, dw_img_ref), (1, dw_txt_ref))]
    for c in stat_copies:
        c.wait_recv()
    total = stats[0]
    for dev in range(1, 16):
        total = total + stats[dev]
    tot_ref[...] = jnp.broadcast_to(jnp.sum(jnp.sum(total, axis=1, keepdims=True), axis=2, keepdims=True), (4, 8, 128))
    for c in shares:
        c.wait_recv()
    for c in write_mine:
        c.start()
    for c in sent + shares + stat_copies:
        c.wait_send()
    for c in write_mine:
        c.wait()


def solution(mesh):
    n_dev = mesh.shape["data"]

    def local_fn(feat_img, feat_txt, w_img, w_txt, log_temp, logit_bias, pair_ids):
        total_rows = feat_img.shape[0] * n_dev
        temp_scale = jnp.exp(log_temp)
        scal = jnp.stack([temp_scale, logit_bias])
        vmem = pl.BlockSpec(memory_space=pltpu.VMEM)
        smem = pl.BlockSpec(memory_space=pltpu.SMEM)
        hbm = pl.BlockSpec(memory_space=pl.ANY)
        dma = pltpu.SemaphoreType.DMA
        part_img, part_txt, sums = pl.pallas_call(
            pair_kernel,
            out_shape=[jax.ShapeDtypeStruct((ROWS, EMBED), F32)] * 2 + [jax.ShapeDtypeStruct((4, 8, 128), F32)],
            in_specs=[smem] + [hbm] * 6,
            out_specs=[hbm, hbm, vmem],
            scratch_shapes=[
                pltpu.VMEM((2, 9, ROWS, EMBED), BF16),
                pltpu.VMEM((9, 1, ROWS), jnp.int32),
                pltpu.VMEM((2 * ROWS, 128), jnp.int32),
                pltpu.VMEM((2, 2 * ROWS, EMBED), F32),
                pltpu.VMEM((2, ROWS, EMBED), F32),
                pltpu.VMEM((TILE_M, ROWS), F32), pltpu.VMEM((TILE_M, ROWS), F32),
                pltpu.VMEM((TILE_M, ROWS), BF16), pltpu.VMEM((TILE_M, ROWS), BF16),
                pltpu.VMEM((4, CHUNK_R, ROWS), F32),
                dma((2, 3, 9)), dma((2, 3, 9)), dma((9,)), dma((9,)), dma((3,)), dma((3,)), dma((2,)), dma((2,)),
                dma((6,)),
            ],
            compiler_params=pltpu.CompilerParams(
                collective_id=0, has_side_effects=True, vmem_limit_bytes=66_000_000),
            cost_estimate=pl.CostEstimate(flops=110_000_000_000, bytes_accessed=16_000_000, transcendentals=0),
        )(scal, feat_img, feat_txt, w_img, w_txt, pair_ids.reshape(1, ROWS),
          jnp.broadcast_to(pair_ids[:, None], (ROWS, 128)))
        dw_img, dw_txt, totals = pl.pallas_call(
            tail_kernel,
            out_shape=[jax.ShapeDtypeStruct((EMBED, EMBED), F32)] * 2 + [jax.ShapeDtypeStruct((4, 8, 128), F32)],
            in_specs=[smem] + [hbm] * 6 + [vmem],
            out_specs=[hbm, hbm, vmem],
            scratch_shapes=[
                pltpu.VMEM((2, ROWS, EMBED), BF16), pltpu.VMEM((2, EMBED, EMBED), BF16),
                pltpu.VMEM((2, ROWS, EMBED), F32), pltpu.VMEM((ROWS, EMBED), BF16),
                pltpu.VMEM((EMBED, EMBED), F32), pltpu.VMEM((2, EMBED, EMBED), F32), pltpu.VMEM((EMBED, EMBED), F32),
                pltpu.VMEM((3, 224, EMBED), F32), pltpu.VMEM((16, 4, 8, 128), F32),
                dma((2, 3)), dma, dma, dma((3, 3)), dma((3, 3)), dma((3, 3)), dma((3, 3)), dma((3, 4)), dma((3, 4)),
                dma((15,)), dma((15,)), pltpu.SemaphoreType.REGULAR,
            ],
            compiler_params=pltpu.CompilerParams(
                collective_id=1, has_side_effects=True, vmem_limit_bytes=60_000_000),
            cost_estimate=pl.CostEstimate(flops=5_000_000_000, bytes_accessed=16_000_000, transcendentals=0),
        )(scal, feat_img, feat_txt, w_img, w_txt, part_img, part_txt, sums)
        loss_sum, temp_sum, bias_sum = totals[0, 0, 0] + totals[1, 0, 0], totals[2, 0, 0], totals[3, 0, 0]
        return loss_sum / total_rows, temp_scale * (temp_sum / total_rows), bias_sum / total_rows, dw_img, dw_txt

    return jax.shard_map(
        local_fn,
        mesh=mesh,
        in_specs=(P("data", None), P("data", None), P(None, None), P(None, None), P(), P(), P("data")),
        out_specs=(P(), P(), P(), P(None, None), P(None, None)),
        check_vma=False,
    )
```

```python
import jax
import jax.numpy as jnp
from jax import lax
from jax.experimental import pallas as pl
from jax.experimental.pallas import tpu as pltpu
from jax.sharding import PartitionSpec as P

F32, BF16 = jnp.float32, jnp.bfloat16
MESH = pl.DeviceIdType.MESH
ROWS, EMBED = 1024, 768
TILE_M, CHUNK_R = 512, 16
LOG2E = 1.4426950408889634
CONTRACT_ROWS = (((0,), (0,)), ((), ()))
CONTRACT_COLS = (((1,), (1,)), ((), ()))

PART_ROWS = ((0, 352), (352, 336), (688, 336))
PART_DIMS = ((1, 2, 4), (2, 4, 1), (4, 1, 2))


def turn_rel(turn, part):
    dims = PART_DIMS[part]
    return {0: dims[0], 1: dims[1], 2: dims[2], 3: dims[0] | dims[1], 4: dims[0] | dims[2], 5: dims[1] | dims[2],
            6: 7}[turn]


SLOT = {(part, turn_rel(turn, part)): 2 + turn for turn in range(7) for part in range(3)}
SLOT.update({(part, 0): 0 for part in range(3)})


def turn_sends(turn):
    ways = {-1: ((None, 0), (None, 1), (None, 2)), 0: ((0, 1), (0, 2)), 1: ((1, 2),), 3: ((3, 2),)}.get(turn, ())
    return [(p, 0 if turn < 0 else turn_rel(turn, p), PART_DIMS[p][k]) for _, k in ways for p in range(3)]


def pair_kernel(scal_ref, feat_img, feat_txt, w_img, w_txt, ids_ref, idrow_ref, dimg_ref, dtxt_ref, sums_ref,
                slots, ids_raw, ids_all, id_rows, acc, partner, s0, s1, g0, g1, sums,
                send_sem, recv_sem, ids_send, ids_recv, pair_send, pair_recv, grad_send, grad_recv, load_sem):
    me = lax.axis_index("data")
    core = me % 2
    chip = me // 2

    def peer(rel):
        where = chip
        for d in (1, 2, 4):
            if rel & d:
                where = where + d * (1 - 2 * ((chip // d) % 2))
        return where * 2 + core

    other_core = chip * 2 + (1 - core)
    loads = [pltpu.make_async_copy(src, slots.at[a, 8], load_sem.at[2 * a]) for a, src in ((0, feat_txt), (1, feat_img))]
    loads += [pltpu.make_async_copy(src, slots.at[a, 7, pl.ds(0, EMBED)], load_sem.at[2 * a + 1])
              for a, src in ((0, w_txt), (1, w_img))]
    loads.append(pltpu.make_async_copy(ids_ref, ids_raw.at[0], load_sem.at[4]))
    loads.append(pltpu.make_async_copy(idrow_ref, id_rows.at[pl.ds(0, ROWS)], load_sem.at[5]))
    for c in loads:
        c.start()
    acc[...] = jnp.zeros_like(acc)
    sums[...] = jnp.zeros_like(sums)
    for c in loads:
        c.wait()

    def embed(i, carry):
        a, rows = i // 2, pl.ds(pl.multiple_of((i % 2) * (ROWS // 2), ROWS // 2), ROWS // 2)
        raw = jnp.dot(slots[a, 8, rows, :], slots[a, 7, 0:EMBED, :], preferred_element_type=F32)
        slots[a, 0, rows, :] = (raw * lax.rsqrt(jnp.sum(raw * raw, axis=1, keepdims=True))).astype(BF16)
        return carry

    lax.fori_loop(0, 4, embed, 0)

    barrier = pltpu.get_barrier_semaphore()
    partners = [other_core] + [peer(rel) for rel in range(1, 8)]
    for dev in partners:
        pl.semaphore_signal(barrier, inc=1, device_id=(dev,), device_id_type=MESH)
    pl.semaphore_wait(barrier, len(partners))

    def part_copy(a, p, rel, d):
        lo, size = PART_ROWS[p]
        return pltpu.make_async_remote_copy(
            src_ref=slots.at[a, SLOT[p, rel], pl.ds(lo, size)],
            dst_ref=slots.at[a, SLOT[p, rel ^ d], pl.ds(lo, size)],
            send_sem=send_sem.at[a, p, SLOT[p, rel ^ d]],
            recv_sem=recv_sem.at[a, p, SLOT[p, rel ^ d]],
            device_id=(peer(d),), device_id_type=MESH)

    def arrival(a, p, rel):
        d = next(x for x in reversed(PART_DIMS[p]) if rel & x)
        part_copy(a, p, rel ^ d, d).wait_recv()

    pair_copies = [pltpu.make_async_remote_copy(
        src_ref=slots.at[a, 0], dst_ref=slots.at[a, 1], send_sem=pair_send.at[a], recv_sem=pair_recv.at[a],
        device_id=(other_core,), device_id_type=MESH) for a in range(2)]
    pair_copies.append(pltpu.make_async_remote_copy(
        src_ref=id_rows.at[pl.ds(0, ROWS)], dst_ref=id_rows.at[pl.ds(ROWS, ROWS)], send_sem=pair_send.at[2],
        recv_sem=pair_recv.at[2], device_id=(other_core,), device_id_type=MESH))
    id_copies = []
    for i, dev in enumerate(partners):
        if i > 0:
            id_copies.append(pltpu.make_async_remote_copy(
                src_ref=ids_raw.at[0], dst_ref=ids_raw.at[i], send_sem=ids_send.at[i],
                recv_sem=ids_recv.at[i], device_id=(dev,), device_id_type=MESH))
    for c in id_copies:
        c.start()
    for c in pair_copies[::-1]:
        c.start()
    for send in turn_sends(-1):
        part_copy(0, *send).start()

    scale, bias = scal_ref[0], scal_ref[1]
    for c in id_copies:
        c.wait_recv()
    lane = lax.broadcasted_iota(jnp.int32, (1, ROWS), 1)
    ids_all[0] = ids_raw[0]
    for turn in range(7):
        ids_all[2 + turn] = jnp.where(
            lane < PART_ROWS[1][0], ids_raw[turn_rel(turn, 0)],
            jnp.where(lane < PART_ROWS[2][0], ids_raw[turn_rel(turn, 1)], ids_raw[turn_rel(turn, 2)]))
    for c in pair_copies:
        c.wait_recv()

    n_m = 2 * ROWS // TILE_M

    def slot_of(block):
        return block + (block + 7) // 8

    def row_tile(t):
        return (t % n_m + (n_m // 2) * ((t // n_m + 7) // 8)) % n_m

    def scores(a, t, s_ref):
        m, slot = pl.multiple_of(row_tile(t) * TILE_M, TILE_M), slot_of(t // n_m)
        rows = slots[1 - a, m // ROWS, pl.ds(pl.multiple_of(m % ROWS, TILE_M), TILE_M), :]
        s_ref[...] = lax.dot_general(rows, slots[a, slot], CONTRACT_COLS, preferred_element_type=F32)

    def tile_grad(a, t, s_ref, g_ref):
        m, slot = pl.multiple_of(row_tile(t) * TILE_M, TILE_M), slot_of(t // n_m)

        col_ids = ids_all[slot]

        def rows_step(i, carry):
            x0, x1 = carry
            top = pl.multiple_of(i * CHUNK_R, CHUNK_R)
            row_ids = jnp.concatenate([id_rows[pl.ds(pl.multiple_of(m + top, CHUNK_R), CHUNK_R), :]] * 8, axis=1)
            sim = s_ref[pl.ds(top, CHUNK_R), :]
            sign = jnp.where(row_ids == col_ids, -1.0, 1.0)
            margin = sign * (scale * sim + bias)
            e = jnp.exp2(jnp.abs(margin) * (-LOG2E))
            d = 1.0 + e
            r = 1.0 / d
            grad = sign * jnp.where(margin >= 0, r, e * r)
            g_ref[pl.ds(top, CHUNK_R), :] = grad.astype(BF16)
            if a == 0:
                return x0 + jnp.maximum(margin, 0.0), x1 * d + e
            return x0 + grad * sim, x1 + grad

        x1 = jnp.zeros((CHUNK_R, ROWS), F32) if a == 0 else sums[3]
        x0, x1 = lax.fori_loop(0, TILE_M // CHUNK_R, rows_step, (sums[2 * a], x1), unroll=True)
        sums[2 * a] = x0
        sums[2 * a + 1] = sums[1] + jnp.log1p(x1) if a == 0 else x1

    def row_grad(a, t, g_ref):
        m, slot = pl.multiple_of(row_tile(t) * TILE_M, TILE_M), slot_of(t // n_m)
        acc[1 - a, pl.ds(m, TILE_M), :] += jnp.dot(g_ref[...], slots[a, slot], preferred_element_type=F32)

    def run_turn(a, turn):
        for p in range(3):
            arrival(a, p, turn_rel(turn, p))
        for send in turn_sends(turn):
            part_copy(a, *send).start()
        if (a, turn) == (0, 3):
            for send in turn_sends(-1):
                part_copy(1, *send).start()

    grad_copies = [pltpu.make_async_remote_copy(
        src_ref=acc.at[x, pl.ds(ROWS, ROWS)], dst_ref=partner.at[x], send_sem=grad_send.at[x],
        recv_sem=grad_recv.at[x], device_id=(other_core,), device_id_type=MESH) for x in range(2)]

    def stream(a):
        t0, t_end = 0, 8 * n_m
        scores(a, t0, s0)
        scores(a, t0 + 1, s1)
        tile_grad(a, t0, s0, g0)

        def body(k, carry):
            t = t0 + 2 * k + 1
            for b in range(1, 8):
                @pl.when(t + 1 == b * n_m)
                def _():
                    run_turn(a, b - 1)
            scores(a, t + 1, s0)
            tile_grad(a, t, s1, g1)
            row_grad(a, t - 1, g0)
            scores(a, t + 2, s1)
            tile_grad(a, t + 1, s0, g0)
            row_grad(a, t, g1)
            return carry

        lax.fori_loop(0, (t_end - t0 - 2) // 2, body, 0)
        grad_copies[1 - a].start()
        tile_grad(a, t_end - 1, s1, g1)
        row_grad(a, t_end - 2, g0)
        row_grad(a, t_end - 1, g1)

    stream(0)
    stream(1)
    grad_copies[1].wait_recv()
    acc[1, 0:ROWS, :] += partner[1]
    outs = [pltpu.make_async_copy(acc.at[x, pl.ds(0, ROWS)], ref, load_sem.at[x]) for x, ref in ((1, dimg_ref), (0, dtxt_ref))]
    outs[0].start()
    for x in range(4):
        rows = sums[x, 0:8, :] + sums[x, 8:16, :]
        sums_ref[x] = sum(rows[:, v:v + 128] for v in range(0, ROWS, 128))
    grad_copies[0].wait_recv()
    acc[0, 0:ROWS, :] += partner[0]
    outs[1].start()
    for c in outs:
        c.wait()
    for c in grad_copies + pair_copies + id_copies:
        c.wait_send()
    for a in range(2):
        for send in [x for turn in (-1, 0, 1, 3) for x in turn_sends(turn)]:
            part_copy(a, *send).wait_send()


def tail_kernel(scal_ref, feat_img, feat_txt, w_img, w_txt, part_img, part_txt, sums_ref, dw_img_ref, dw_txt_ref, tot_ref,
                feats, heads, parts, raw_grad, mine, full, from_core, landing, stats,
                load_sem, core_send, core_recv, rs_send, rs_recv, ag_send, ag_recv, out_send, out_recv, st_send, st_recv, ready):
    me = lax.axis_index("data")
    core, chip = me % 2, me // 2
    other_core = chip * 2 + (1 - core)
    near = {d: (chip + d * (1 - 2 * ((chip // d) % 2))) * 2 + core for d in (1, 2, 4)}
    others = [(me + k) % 16 for k in range(1, 16)]

    loads = []
    for a, refs in enumerate(((feat_img, w_img, part_img), (feat_txt, w_txt, part_txt))):
        loads += [pltpu.make_async_copy(src, dst.at[a], load_sem.at[a, k])
                  for k, (src, dst) in enumerate(zip(refs, (feats, heads, parts)))]
    for c in loads:
        c.start()
    barrier = pltpu.get_barrier_semaphore()
    for dev in others:
        pl.semaphore_signal(barrier, inc=1, device_id=(dev,), device_id_type=MESH)
    for c in loads:
        c.wait()
    scale = scal_ref[0]
    total_rows = 16 * ROWS

    def head_grad(a, dst):
        def rows_step(i, carry):
            rows = pl.ds(pl.multiple_of(i * 256, 256), 256)
            raw = jnp.dot(feats[a, rows, :], heads[a], preferred_element_type=F32)
            inv = lax.rsqrt(jnp.sum(raw * raw, axis=1, keepdims=True))
            unit = raw * inv
            grad = scale * (parts[a, rows, :] * F32(1.0 / total_rows))
            raw_grad[rows, :] = (inv * (grad - unit * jnp.sum(unit * grad, axis=1, keepdims=True))).astype(BF16)
            return carry

        lax.fori_loop(0, ROWS // 256, rows_step, 0)
        dst[...] = lax.dot_general(feats[a], raw_grad[...], CONTRACT_ROWS, preferred_element_type=F32)

    head_grad(1 - core, full.at[1 - core])
    pl.semaphore_wait(barrier, len(others))
    to_core = pltpu.make_async_remote_copy(
        src_ref=full.at[1 - core], dst_ref=from_core, send_sem=core_send, recv_sem=core_recv,
        device_id=(other_core,), device_id_type=MESH)
    to_core.start()
    stats[me] = sums_ref[...]
    stat_copies = [pltpu.make_async_remote_copy(
        src_ref=stats.at[me], dst_ref=stats.at[me], send_sem=st_send.at[k], recv_sem=st_recv.at[k],
        device_id=(dev,), device_id_type=MESH) for k, dev in enumerate(others)]
    for c in stat_copies:
        c.start()
    head_grad(core, mine)
    to_core.wait_recv()
    mine[...] += from_core[...]

    bits = [[(chip // PART_DIMS[p][k]) % 2 for k in range(3)] for p in range(3)]
    lows = [[256 * p] for p in range(3)]
    for p in range(3):
        for k, half in enumerate((128, 64, 32)):
            lows[p].append(lows[p][-1] + bits[p][k] * half)
    halves = [pl.ds(h * (EMBED // 2), EMBED // 2) for h in range(2)]
    sent = []

    def scatter_copy(k, p, h):
        half = (128, 64, 32)[k]
        src = pl.multiple_of(lows[p][k] + (1 - bits[p][k]) * half, 32)
        return pltpu.make_async_remote_copy(
            src_ref=mine.at[pl.ds(src, half), halves[h]], dst_ref=landing.at[p, pl.ds((0, 128, 192)[k], half), halves[h]],
            send_sem=rs_send.at[k, p, h], recv_sem=rs_recv.at[k, p, h], device_id=(near[PART_DIMS[p][k]],),
            device_id_type=MESH)

    for h in range(2):
        for p in range(3):
            scatter_copy(0, p, h).start()
    for k, half in enumerate((128, 64, 32)):
        for h in range(2):
            for p in range(3):
                scatter_copy(k, p, h).wait_recv()
                rows = pl.ds(pl.multiple_of(lows[p][k + 1], 32), half)
                base = (0, 128, 192)[k]
                total = mine[rows, halves[h]] + landing[p, base:base + half, halves[h]]
                if k < 2:
                    mine[rows, halves[h]] = total
                    scatter_copy(k + 1, p, h).start()
                else:
                    full[core, rows, halves[h]] = total
                sent.append(scatter_copy(k, p, h))

    def share(low, size, p, k, h):
        rows = pl.ds(pl.multiple_of(low, 32), size)
        return pltpu.make_async_remote_copy(
            src_ref=full.at[core, rows, halves[h]], dst_ref=full.at[core, rows, halves[h]], send_sem=out_send.at[p, k, h],
            recv_sem=out_recv.at[p, k, h], device_id=(other_core,), device_id_type=MESH)

    def gather_copy(k, p, h):
        rows = pl.ds(pl.multiple_of(lows[p][k + 1], 32), (128, 64, 32)[k])
        return pltpu.make_async_remote_copy(
            src_ref=full.at[core, rows, halves[h]], dst_ref=full.at[core, rows, halves[h]], send_sem=ag_send.at[k, p, h],
            recv_sem=ag_recv.at[k, p, h], device_id=(near[PART_DIMS[p][k]],), device_id_type=MESH)

    to_core.wait_send()
    pl.semaphore_signal(ready, inc=1, device_id=(other_core,), device_id_type=MESH)
    pl.semaphore_wait(ready, 1)
    shares = []
    for h in range(2):
        for p in range(3):
            gather_copy(2, p, h).start()
            shares.append(share(lows[p][3], 32, p, 3, h))
            shares[-1].start()
    for k in (2, 1, 0):
        for h in range(2):
            for p in range(3):
                size = (128, 64, 32)[k]
                gather_copy(k, p, h).wait_recv()
                if k > 0:
                    gather_copy(k - 1, p, h).start()
                shares.append(share(lows[p][k] + (1 - bits[p][k]) * size, size, p, k, h))
                shares[-1].start()
                sent.append(gather_copy(k, p, h))
    write_mine = [pltpu.make_async_copy(full.at[a], ref, load_sem.at[a, 0]) for a, ref in ((0, dw_img_ref), (1, dw_txt_ref))]
    for c in stat_copies:
        c.wait_recv()
    total = stats[0]
    for dev in range(1, 16):
        total = total + stats[dev]
    tot_ref[...] = jnp.broadcast_to(jnp.sum(jnp.sum(total, axis=1, keepdims=True), axis=2, keepdims=True), (4, 8, 128))
    for c in shares:
        c.wait_recv()
    for c in write_mine:
        c.start()
    for c in sent + shares + stat_copies:
        c.wait_send()
    for c in write_mine:
        c.wait()


def solution(mesh):
    n_dev = mesh.shape["data"]

    def local_fn(feat_img, feat_txt, w_img, w_txt, log_temp, logit_bias, pair_ids):
        total_rows = feat_img.shape[0] * n_dev
        temp_scale = jnp.exp(log_temp)
        scal = jnp.stack([temp_scale, logit_bias])
        vmem = pl.BlockSpec(memory_space=pltpu.VMEM)
        smem = pl.BlockSpec(memory_space=pltpu.SMEM)
        hbm = pl.BlockSpec(memory_space=pl.ANY)
        dma = pltpu.SemaphoreType.DMA
        part_img, part_txt, sums = pl.pallas_call(
            pair_kernel,
            out_shape=[jax.ShapeDtypeStruct((ROWS, EMBED), F32)] * 2 + [jax.ShapeDtypeStruct((4, 8, 128), F32)],
            in_specs=[smem] + [hbm] * 6,
            out_specs=[hbm, hbm, vmem],
            scratch_shapes=[
                pltpu.VMEM((2, 9, ROWS, EMBED), BF16),
                pltpu.VMEM((8, 1, ROWS), jnp.int32), pltpu.VMEM((9, 1, ROWS), jnp.int32),
                pltpu.VMEM((2 * ROWS, 128), jnp.int32),
                pltpu.VMEM((2, 2 * ROWS, EMBED), F32),
                pltpu.VMEM((2, ROWS, EMBED), F32),
                pltpu.VMEM((TILE_M, ROWS), F32), pltpu.VMEM((TILE_M, ROWS), F32),
                pltpu.VMEM((TILE_M, ROWS), BF16), pltpu.VMEM((TILE_M, ROWS), BF16),
                pltpu.VMEM((4, CHUNK_R, ROWS), F32),
                dma((2, 3, 9)), dma((2, 3, 9)), dma((9,)), dma((9,)), dma((3,)), dma((3,)), dma((2,)), dma((2,)),
                dma((6,)),
            ],
            compiler_params=pltpu.CompilerParams(
                collective_id=0, has_side_effects=True, vmem_limit_bytes=66_000_000),
            cost_estimate=pl.CostEstimate(flops=110_000_000_000, bytes_accessed=16_000_000, transcendentals=0),
        )(scal, feat_img, feat_txt, w_img, w_txt, pair_ids.reshape(1, ROWS),
          jnp.broadcast_to(pair_ids[:, None], (ROWS, 128)))
        dw_img, dw_txt, totals = pl.pallas_call(
            tail_kernel,
            out_shape=[jax.ShapeDtypeStruct((EMBED, EMBED), F32)] * 2 + [jax.ShapeDtypeStruct((4, 8, 128), F32)],
            in_specs=[smem] + [hbm] * 6 + [vmem],
            out_specs=[hbm, hbm, vmem],
            scratch_shapes=[
                pltpu.VMEM((2, ROWS, EMBED), BF16), pltpu.VMEM((2, EMBED, EMBED), BF16),
                pltpu.VMEM((2, ROWS, EMBED), F32), pltpu.VMEM((ROWS, EMBED), BF16),
                pltpu.VMEM((EMBED, EMBED), F32), pltpu.VMEM((2, EMBED, EMBED), F32), pltpu.VMEM((EMBED, EMBED), F32),
                pltpu.VMEM((3, 224, EMBED), F32), pltpu.VMEM((16, 4, 8, 128), F32),
                dma((2, 3)), dma, dma, dma((3, 3, 2)), dma((3, 3, 2)), dma((3, 3, 2)), dma((3, 3, 2)), dma((3, 4, 2)),
                dma((3, 4, 2)),
                dma((15,)), dma((15,)), pltpu.SemaphoreType.REGULAR,
            ],
            compiler_params=pltpu.CompilerParams(
                collective_id=1, has_side_effects=True, vmem_limit_bytes=60_000_000),
            cost_estimate=pl.CostEstimate(flops=5_000_000_000, bytes_accessed=16_000_000, transcendentals=0),
        )(scal, feat_img, feat_txt, w_img, w_txt, part_img, part_txt, sums)
        loss_sum, temp_sum, bias_sum = totals[0, 0, 0] + totals[1, 0, 0], totals[2, 0, 0], totals[3, 0, 0]
        return loss_sum / total_rows, temp_scale * (temp_sum / total_rows), bias_sum / total_rows, dw_img, dw_txt

    return jax.shard_map(
        local_fn,
        mesh=mesh,
        in_specs=(P("data", None), P("data", None), P(None, None), P(None, None), P(), P(), P("data")),
        out_specs=(P(), P(), P(), P(None, None), P(None, None)),
        check_vma=False,
    )
```

```python
import jax
import jax.numpy as jnp
from jax import lax
from jax.experimental import pallas as pl
from jax.experimental.pallas import tpu as pltpu
from jax.sharding import PartitionSpec as P

F32, BF16 = jnp.float32, jnp.bfloat16
MESH = pl.DeviceIdType.MESH
ROWS, EMBED = 1024, 768
TILE_M, CHUNK_R = 512, 16
LOG2E = 1.4426950408889634
CONTRACT_ROWS = (((0,), (0,)), ((), ()))
CONTRACT_COLS = (((1,), (1,)), ((), ()))

PART_ROWS = ((0, 352), (352, 336), (688, 336))
PART_DIMS = ((1, 2, 4), (2, 4, 1), (4, 1, 2))


def turn_rel(turn, part):
    dims = PART_DIMS[part]
    return {0: dims[0], 1: dims[1], 2: dims[2], 3: dims[0] | dims[1], 4: dims[0] | dims[2], 5: dims[1] | dims[2],
            6: 7}[turn]


SLOT = {(part, turn_rel(turn, part)): 2 + turn for turn in range(7) for part in range(3)}
SLOT.update({(part, 0): 0 for part in range(3)})


def turn_sends(turn):
    ways = {-1: ((None, 0), (None, 1), (None, 2)), 0: ((0, 1), (0, 2)), 1: ((1, 2),), 3: ((3, 2),)}.get(turn, ())
    return [(p, 0 if turn < 0 else turn_rel(turn, p), PART_DIMS[p][k]) for _, k in ways for p in range(3)]


def pair_kernel(scal_ref, feat_img, feat_txt, w_img, w_txt, ids_ref, idrow_ref, dw_img_ref, dw_txt_ref, tot_ref,
                slots, ids_raw, ids_all, id_rows, acc, partner, s0, s1, g0, g1, sums, stats,
                send_sem, recv_sem, ids_send, ids_recv, pair_send, pair_recv, grad_send, grad_recv, load_sem,
                late_sem, core_send, core_recv, rs_send, rs_recv, ag_send, ag_recv, out_send, out_recv, st_send, st_recv, ready):
    me = lax.axis_index("data")
    core = me % 2
    chip = me // 2

    def peer(rel):
        where = chip
        for d in (1, 2, 4):
            if rel & d:
                where = where + d * (1 - 2 * ((chip // d) % 2))
        return where * 2 + core

    other_core = chip * 2 + (1 - core)
    loads = [pltpu.make_async_copy(src, slots.at[a, 8], load_sem.at[2 * a]) for a, src in ((0, feat_txt), (1, feat_img))]
    loads += [pltpu.make_async_copy(src, slots.at[a, 7, pl.ds(0, EMBED)], load_sem.at[2 * a + 1])
              for a, src in ((0, w_txt), (1, w_img))]
    loads.append(pltpu.make_async_copy(ids_ref, ids_raw.at[0], load_sem.at[4]))
    loads.append(pltpu.make_async_copy(idrow_ref, id_rows.at[pl.ds(0, ROWS)], load_sem.at[5]))
    for c in loads:
        c.start()
    acc[...] = jnp.zeros_like(acc)
    sums[...] = jnp.zeros_like(sums)
    for c in loads:
        c.wait()

    def embed(i, carry):
        a, rows = i // 2, pl.ds(pl.multiple_of((i % 2) * (ROWS // 2), ROWS // 2), ROWS // 2)
        raw = jnp.dot(slots[a, 8, rows, :], slots[a, 7, 0:EMBED, :], preferred_element_type=F32)
        slots[a, 0, rows, :] = (raw * lax.rsqrt(jnp.sum(raw * raw, axis=1, keepdims=True))).astype(BF16)
        return carry

    lax.fori_loop(0, 4, embed, 0)

    barrier = pltpu.get_barrier_semaphore()
    others = [(me + k) % 16 for k in range(1, 16)]
    for dev in others:
        pl.semaphore_signal(barrier, inc=1, device_id=(dev,), device_id_type=MESH)
    pl.semaphore_wait(barrier, len(others))

    def part_copy(a, p, rel, d):
        lo, size = PART_ROWS[p]
        return pltpu.make_async_remote_copy(
            src_ref=slots.at[a, SLOT[p, rel], pl.ds(lo, size)],
            dst_ref=slots.at[a, SLOT[p, rel ^ d], pl.ds(lo, size)],
            send_sem=send_sem.at[a, p, SLOT[p, rel ^ d]],
            recv_sem=recv_sem.at[a, p, SLOT[p, rel ^ d]],
            device_id=(peer(d),), device_id_type=MESH)

    def arrival(a, p, rel):
        d = next(x for x in reversed(PART_DIMS[p]) if rel & x)
        part_copy(a, p, rel ^ d, d).wait_recv()

    pair_copies = [pltpu.make_async_remote_copy(
        src_ref=slots.at[a, 0], dst_ref=slots.at[a, 1], send_sem=pair_send.at[a], recv_sem=pair_recv.at[a],
        device_id=(other_core,), device_id_type=MESH) for a in range(2)]
    pair_copies.append(pltpu.make_async_remote_copy(
        src_ref=id_rows.at[pl.ds(0, ROWS)], dst_ref=id_rows.at[pl.ds(ROWS, ROWS)], send_sem=pair_send.at[2],
        recv_sem=pair_recv.at[2], device_id=(other_core,), device_id_type=MESH))
    id_copies = []
    for rel in range(1, 8):
        id_copies.append(pltpu.make_async_remote_copy(
            src_ref=ids_raw.at[0], dst_ref=ids_raw.at[rel], send_sem=ids_send.at[rel],
            recv_sem=ids_recv.at[rel], device_id=(peer(rel),), device_id_type=MESH))
    for c in id_copies:
        c.start()
    for c in pair_copies[::-1]:
        c.start()
    for send in turn_sends(-1):
        part_copy(0, *send).start()

    scale, bias = scal_ref[0], scal_ref[1]
    for c in id_copies:
        c.wait_recv()
    lane = lax.broadcasted_iota(jnp.int32, (1, ROWS), 1)
    ids_all[0] = ids_raw[0]
    for turn in range(7):
        ids_all[2 + turn] = jnp.where(
            lane < PART_ROWS[1][0], ids_raw[turn_rel(turn, 0)],
            jnp.where(lane < PART_ROWS[2][0], ids_raw[turn_rel(turn, 1)], ids_raw[turn_rel(turn, 2)]))
    for c in pair_copies:
        c.wait_recv()

    n_m = 2 * ROWS // TILE_M

    def slot_of(block):
        return block + (block + 7) // 8

    def row_tile(t):
        return (t % n_m + (n_m // 2) * ((t // n_m + 7) // 8)) % n_m

    def scores(a, t, s_ref):
        m, slot = pl.multiple_of(row_tile(t) * TILE_M, TILE_M), slot_of(t // n_m)
        rows = slots[1 - a, m // ROWS, pl.ds(pl.multiple_of(m % ROWS, TILE_M), TILE_M), :]
        s_ref[...] = lax.dot_general(rows, slots[a, slot], CONTRACT_COLS, preferred_element_type=F32)

    def tile_grad(a, t, s_ref, g_ref):
        m, slot = pl.multiple_of(row_tile(t) * TILE_M, TILE_M), slot_of(t // n_m)

        col_ids = ids_all[slot]

        def rows_step(i, carry):
            x0, x1 = carry
            top = pl.multiple_of(i * CHUNK_R, CHUNK_R)
            row_ids = jnp.concatenate([id_rows[pl.ds(pl.multiple_of(m + top, CHUNK_R), CHUNK_R), :]] * 8, axis=1)
            sim = s_ref[pl.ds(top, CHUNK_R), :]
            sign = jnp.where(row_ids == col_ids, -1.0, 1.0)
            margin = sign * (scale * sim + bias)
            e = jnp.exp2(jnp.abs(margin) * (-LOG2E))
            d = 1.0 + e
            r = 1.0 / d
            grad = sign * jnp.where(margin >= 0, r, e * r)
            g_ref[pl.ds(top, CHUNK_R), :] = grad.astype(BF16)
            if a == 0:
                return x0 + jnp.maximum(margin, 0.0), x1 * d + e
            return x0 + grad * sim, x1 + grad

        x1 = jnp.zeros((CHUNK_R, ROWS), F32) if a == 0 else sums[3]
        x0, x1 = lax.fori_loop(0, TILE_M // CHUNK_R, rows_step, (sums[2 * a], x1), unroll=True)
        sums[2 * a] = x0
        sums[2 * a + 1] = sums[1] + jnp.log1p(x1) if a == 0 else x1

    def row_grad(a, t, g_ref):
        m, slot = pl.multiple_of(row_tile(t) * TILE_M, TILE_M), slot_of(t // n_m)
        acc[1 - a, pl.ds(m, TILE_M), :] += jnp.dot(g_ref[...], slots[a, slot], preferred_element_type=F32)

    def run_turn(a, turn):
        for p in range(3):
            arrival(a, p, turn_rel(turn, p))
        for send in turn_sends(turn):
            part_copy(a, *send).start()
        if (a, turn) == (0, 3):
            for send in turn_sends(-1):
                part_copy(1, *send).start()

    grad_copies = [pltpu.make_async_remote_copy(
        src_ref=acc.at[x, pl.ds(ROWS, ROWS)], dst_ref=partner.at[x], send_sem=grad_send.at[x],
        recv_sem=grad_recv.at[x], device_id=(other_core,), device_id_type=MESH) for x in range(2)]

    def stream(a):
        t0, t_end = 0, 8 * n_m
        scores(a, t0, s0)
        scores(a, t0 + 1, s1)
        tile_grad(a, t0, s0, g0)

        def body(k, carry):
            t = t0 + 2 * k + 1
            for task, todo in actions[a].items():
                @pl.when(t + 1 == task)
                def _():
                    for act in todo:
                        act()
            scores(a, t + 1, s0)
            tile_grad(a, t, s1, g1)
            row_grad(a, t - 1, g0)
            scores(a, t + 2, s1)
            tile_grad(a, t + 1, s0, g0)
            row_grad(a, t, g1)
            return carry

        lax.fori_loop(0, (t_end - t0 - 2) // 2, body, 0)
        grad_copies[1 - a].start()
        tile_grad(a, t_end - 1, s1, g1)
        row_grad(a, t_end - 2, g0)
        row_grad(a, t_end - 1, g1)

    half_rows = EMBED // 2
    steps = (64, 32, 16)
    bits = [[(chip // PART_DIMS[p][k]) % 2 for k in range(3)] for p in range(3)]
    lows = [[core * half_rows + 128 * p] for p in range(3)]
    for p in range(3):
        for k in range(3):
            lows[p].append(lows[p][-1] + bits[p][k] * steps[k])
    cols = [pl.ds(h * (EMBED // 2), EMBED // 2) for h in range(2)]
    lanes = [(p, h) for h in range(2) for p in range(3)]
    started = []

    def start(make, *args):
        make(*args).start()
        started.append((make, args))

    def rows_at(low, size, base=0):
        return pl.ds(pl.multiple_of(low + base, 16), size)

    def near(p, k):
        return (peer(PART_DIMS[p][k]),)

    def core_copy(x):
        return pltpu.make_async_remote_copy(
            src_ref=acc.at[x, rows_at((1 - core) * half_rows, half_rows, ROWS)], dst_ref=partner.at[x, pl.ds(0, half_rows)],
            send_sem=core_send.at[x], recv_sem=core_recv.at[x], device_id=(other_core,), device_id_type=MESH)

    def scatter_copy(x, k, p, h):
        return pltpu.make_async_remote_copy(
            src_ref=acc.at[x, rows_at(lows[p][k] + (1 - bits[p][k]) * steps[k], steps[k], ROWS), cols[h]],
            dst_ref=partner.at[x, pl.ds(half_rows + 112 * p + (0, 64, 96)[k], steps[k]), cols[h]],
            send_sem=rs_send.at[x, k, p, h], recv_sem=rs_recv.at[x, k, p, h], device_id=near(p, k), device_id_type=MESH)

    def gather_copy(x, k, p, h):
        rows = rows_at(lows[p][k + 1], steps[k])
        return pltpu.make_async_remote_copy(
            src_ref=acc.at[x, rows, cols[h]], dst_ref=acc.at[x, rows, cols[h]], send_sem=ag_send.at[x, k, p, h],
            recv_sem=ag_recv.at[x, k, p, h], device_id=near(p, k), device_id_type=MESH)

    def share(x, k, p, h):
        rows = rows_at(lows[p][3], 16) if k == 3 else rows_at(lows[p][k] + (1 - bits[p][k]) * steps[k], steps[k])
        return pltpu.make_async_remote_copy(
            src_ref=acc.at[x, rows, cols[h]], dst_ref=acc.at[x, rows, cols[h]], send_sem=out_send.at[x, k, p, h],
            recv_sem=out_recv.at[x, k, p, h], device_id=(other_core,), device_id_type=MESH)

    def late_load(x):
        srcs = ((feat_txt, slots.at[0, 5]), (w_txt, slots.at[0, 6, pl.ds(0, EMBED)])) if x == 0 else (
            (feat_img, slots.at[0, 2]), (w_img, slots.at[0, 3, pl.ds(0, EMBED)]))
        return [pltpu.make_async_copy(src, dst, late_sem.at[x, k]) for k, (src, dst) in enumerate(srcs)]

    def begin_load(x, turns):
        for turn in turns:
            for send in turn_sends(turn):
                part_copy(0, *send).wait_send()
        for c in late_load(x):
            c.start()

    def head_partial(x):
        for c in late_load(x):
            c.wait()
        feat, head = (5, 6) if x == 0 else (2, 3)

        def rows_step(i, carry):
            rows = pl.ds(pl.multiple_of(i * 256, 256), 256)
            raw = jnp.dot(slots[0, feat, rows, :], slots[0, head, 0:EMBED, :], preferred_element_type=F32)
            inv = lax.rsqrt(jnp.sum(raw * raw, axis=1, keepdims=True))
            unit = raw * inv
            grad = scale * ((acc[x, rows, :] + partner[x, rows, :]) * F32(1.0 / (16 * ROWS)))
            slots[0, 4, rows, :] = (inv * (grad - unit * jnp.sum(unit * grad, axis=1, keepdims=True))).astype(BF16)
            return carry

        lax.fori_loop(0, ROWS // 256, rows_step, 0)
        grad_copies[x].wait_send()
        acc[x, ROWS:ROWS + EMBED, :] = lax.dot_general(
            slots[0, feat], slots[0, 4], CONTRACT_ROWS, preferred_element_type=F32)
        for dev in [other_core] + [peer(d) for d in (1, 2, 4)]:
            pl.semaphore_signal(ready.at[x], inc=1, device_id=(dev,), device_id_type=MESH)

    def step_core(x):
        pl.semaphore_wait(ready.at[x], 4)
        start(core_copy, x)

    def step_first(x):
        core_copy(x).wait_recv()
        acc[x, rows_at(core * half_rows, half_rows, ROWS), :] += partner[x, 0:half_rows, :]
        for p, h in lanes:
            start(scatter_copy, x, 0, p, h)

    def step_scatter(x, k):
        for p, h in lanes:
            scatter_copy(x, k, p, h).wait_recv()
            base = half_rows + 112 * p + (0, 64, 96)[k]
            mine = rows_at(lows[p][k + 1], steps[k], ROWS)
            total = acc[x, mine, cols[h]] + partner[x, base:base + steps[k], cols[h]]
            if k < 2:
                acc[x, mine, cols[h]] = total
                start(scatter_copy, x, k + 1, p, h)
            else:
                acc[x, rows_at(lows[p][3], 16), cols[h]] = total
                start(gather_copy, x, 2, p, h)
                start(share, x, 3, p, h)

    def step_gather(x, k):
        for p, h in lanes:
            gather_copy(x, k, p, h).wait_recv()
            if k > 0:
                start(gather_copy, x, k - 1, p, h)
            start(share, x, k, p, h)

    def step_out(x):
        for k in (3, 2, 1, 0):
            for p, h in lanes:
                share(x, k, p, h).wait_recv()
        outs[x].start()

    outs = [pltpu.make_async_copy(acc.at[x, pl.ds(0, EMBED)], ref, load_sem.at[x])
            for x, ref in ((0, dw_txt_ref), (1, dw_img_ref))]
    actions = [{b * n_m: [lambda a=a, b=b: run_turn(a, b - 1)] for b in range(1, 8)} for a in range(2)]
    actions[0][7 * n_m].append(lambda: begin_load(1, (-1, 0, 1)))
    actions[1][n_m].append(lambda: (step_core(1), begin_load(0, (3,))))
    actions[1][5 * n_m].append(lambda: step_first(1))
    actions[1][7 * n_m + 2] = [lambda: step_scatter(1, 0)]

    stream(0)
    grad_copies[1].wait_recv()
    head_partial(1)
    stream(1)
    step_scatter(1, 1)
    for x in range(4):
        rows = sums[x, 0:8, :] + sums[x, 8:16, :]
        stats[me, x] = sum(rows[:, v:v + 128] for v in range(0, ROWS, 128))
    stat_copies = [pltpu.make_async_remote_copy(
        src_ref=stats.at[me], dst_ref=stats.at[me], send_sem=st_send.at[k], recv_sem=st_recv.at[k],
        device_id=(dev,), device_id_type=MESH) for k, dev in enumerate(others)]
    grad_copies[0].wait_recv()
    step_scatter(1, 2)
    head_partial(0)
    for c in stat_copies:
        c.start()
    step_core(0)
    step_gather(1, 2)
    step_first(0)
    step_gather(1, 1)
    step_scatter(0, 0)
    step_gather(1, 0)
    step_scatter(0, 1)
    step_out(1)
    step_scatter(0, 2)
    for c in stat_copies:
        c.wait_recv()
    total = stats[0]
    for dev in range(1, 16):
        total = total + stats[dev]
    tot_ref[...] = jnp.broadcast_to(jnp.sum(jnp.sum(total, axis=1, keepdims=True), axis=2, keepdims=True), (4, 8, 128))
    for k in (2, 1, 0):
        step_gather(0, k)
    step_out(0)
    for c in pair_copies + id_copies + stat_copies:
        c.wait_send()
    for make, args in started:
        make(*args).wait_send()
    for turn in (-1, 0, 1, 3):
        for send in turn_sends(turn):
            part_copy(1, *send).wait_send()
    for c in outs:
        c.wait()


def solution(mesh):
    n_dev = mesh.shape["data"]

    def local_fn(feat_img, feat_txt, w_img, w_txt, log_temp, logit_bias, pair_ids):
        total_rows = feat_img.shape[0] * n_dev
        temp_scale = jnp.exp(log_temp)
        scal = jnp.stack([temp_scale, logit_bias])
        vmem = pl.BlockSpec(memory_space=pltpu.VMEM)
        smem = pl.BlockSpec(memory_space=pltpu.SMEM)
        hbm = pl.BlockSpec(memory_space=pl.ANY)
        dma = pltpu.SemaphoreType.DMA
        dw_img, dw_txt, totals = pl.pallas_call(
            pair_kernel,
            out_shape=[jax.ShapeDtypeStruct((EMBED, EMBED), F32)] * 2 + [jax.ShapeDtypeStruct((4, 8, 128), F32)],
            in_specs=[smem] + [hbm] * 6,
            out_specs=[hbm, hbm, vmem],
            scratch_shapes=[
                pltpu.VMEM((2, 9, ROWS, EMBED), BF16),
                pltpu.VMEM((8, 1, ROWS), jnp.int32), pltpu.VMEM((9, 1, ROWS), jnp.int32),
                pltpu.VMEM((2 * ROWS, 128), jnp.int32),
                pltpu.VMEM((2, 2 * ROWS, EMBED), F32),
                pltpu.VMEM((2, ROWS, EMBED), F32),
                pltpu.VMEM((TILE_M, ROWS), F32), pltpu.VMEM((TILE_M, ROWS), F32),
                pltpu.VMEM((TILE_M, ROWS), BF16), pltpu.VMEM((TILE_M, ROWS), BF16),
                pltpu.VMEM((4, CHUNK_R, ROWS), F32), pltpu.VMEM((16, 4, 8, 128), F32),
                dma((2, 3, 9)), dma((2, 3, 9)), dma((9,)), dma((9,)), dma((3,)), dma((3,)), dma((2,)), dma((2,)),
                dma((6,)), dma((2, 2)), dma((2,)), dma((2,)), dma((2, 3, 3, 2)), dma((2, 3, 3, 2)), dma((2, 3, 3, 2)),
                dma((2, 3, 3, 2)), dma((2, 4, 3, 2)), dma((2, 4, 3, 2)), dma((15,)), dma((15,)),
                pltpu.SemaphoreType.REGULAR((2,)),
            ],
            compiler_params=pltpu.CompilerParams(
                collective_id=0, has_side_effects=True, vmem_limit_bytes=66_000_000),
            cost_estimate=pl.CostEstimate(flops=110_000_000_000, bytes_accessed=16_000_000, transcendentals=0),
        )(scal, feat_img, feat_txt, w_img, w_txt, pair_ids.reshape(1, ROWS),
          jnp.broadcast_to(pair_ids[:, None], (ROWS, 128)))
        loss_sum, temp_sum, bias_sum = totals[0, 0, 0] + totals[1, 0, 0], totals[2, 0, 0], totals[3, 0, 0]
        return loss_sum / total_rows, temp_scale * (temp_sum / total_rows), bias_sum / total_rows, dw_img, dw_txt

    return jax.shard_map(
        local_fn,
        mesh=mesh,
        in_specs=(P("data", None), P("data", None), P(None, None), P(None, None), P(), P(), P("data")),
        out_specs=(P(), P(), P(), P(None, None), P(None, None)),
        check_vma=False,
    )
```

```python
import jax
import jax.numpy as jnp
from jax import lax
from jax.experimental import pallas as pl
from jax.experimental.pallas import tpu as pltpu
from jax.sharding import PartitionSpec as P

F32, BF16 = jnp.float32, jnp.bfloat16
MESH = pl.DeviceIdType.MESH
ROWS, EMBED = 1024, 768
TILE_M, CHUNK_R = 512, 16
LOG2E = 1.4426950408889634
CONTRACT_ROWS = (((0,), (0,)), ((), ()))
CONTRACT_COLS = (((1,), (1,)), ((), ()))

PART_ROWS = ((0, 352), (352, 336), (688, 336))
PART_DIMS = ((1, 2, 4), (2, 4, 1), (4, 1, 2))


def turn_rel(turn, part):
    dims = PART_DIMS[part]
    return {0: dims[0], 1: dims[1], 2: dims[2], 3: dims[0] | dims[1], 4: dims[0] | dims[2], 5: dims[1] | dims[2],
            6: 7}[turn]


SLOT = {(part, turn_rel(turn, part)): 2 + turn for turn in range(7) for part in range(3)}
SLOT.update({(part, 0): 0 for part in range(3)})


def own_sends(k):
    return [(p, 0, PART_DIMS[p][k]) for p in range(3)]


def turn_sends(turn):
    ways = {-1: ((None, 0), (None, 1), (None, 2)), 0: ((0, 1), (0, 2)), 1: ((1, 2),), 3: ((3, 2),)}.get(turn, ())
    return [(p, 0 if turn < 0 else turn_rel(turn, p), PART_DIMS[p][k]) for _, k in ways for p in range(3)]


def pair_kernel(scal_ref, feat_img, feat_txt, w_img, w_txt, ids_ref, idrow_ref, dw_img_ref, dw_txt_ref, tot_ref,
                slots, ids_raw, ids_all, id_rows, acc, partner, s0, s1, g0, g1, sums, stats, head,
                send_sem, recv_sem, ids_send, ids_recv, pair_send, pair_recv, grad_send, grad_recv, load_sem,
                late_sem, core_send, core_recv, rs_send, rs_recv, ag_send, ag_recv, out_send, out_recv, st_send, st_recv, ready):
    me = lax.axis_index("data")
    core = me % 2
    chip = me // 2

    def peer(rel):
        where = chip
        for d in (1, 2, 4):
            if rel & d:
                where = where + d * (1 - 2 * ((chip // d) % 2))
        return where * 2 + core

    other_core = chip * 2 + (1 - core)
    txt_loads = [pltpu.make_async_copy(feat_txt, slots.at[0, 8], load_sem.at[0]),
                 pltpu.make_async_copy(w_txt, slots.at[0, 7, pl.ds(0, EMBED)], load_sem.at[1])]
    img_loads = [pltpu.make_async_copy(feat_img.at[pl.ds(0, TILE_M)], g0.at[:, pl.ds(0, EMBED)], load_sem.at[2]),
                 pltpu.make_async_copy(feat_img.at[pl.ds(TILE_M, TILE_M)], g1.at[:, pl.ds(0, EMBED)], load_sem.at[3]),
                 pltpu.make_async_copy(w_img, head, load_sem.at[4]),
                 pltpu.make_async_copy(ids_ref, ids_raw.at[0], load_sem.at[5]),
                 pltpu.make_async_copy(idrow_ref, id_rows.at[pl.ds(0, ROWS)], load_sem.at[6])]
    for c in txt_loads + img_loads:
        c.start()
    for c in txt_loads:
        c.wait()

    def unit_rows(feat_rows, weights):
        raw = jnp.dot(feat_rows, weights, preferred_element_type=F32)
        return (raw * lax.rsqrt(jnp.sum(raw * raw, axis=1, keepdims=True))).astype(BF16)

    def embed_txt(i, carry):
        rows = pl.ds(pl.multiple_of(i * TILE_M, TILE_M), TILE_M)
        slots[0, 0, rows, :] = unit_rows(slots[0, 8, rows, :], slots[0, 7, 0:EMBED, :])
        return carry

    lax.fori_loop(0, ROWS // TILE_M, embed_txt, 0)

    barrier = pltpu.get_barrier_semaphore()
    others = [(me + k) % 16 for k in range(1, 16)]
    for dev in others:
        pl.semaphore_signal(barrier, inc=1, device_id=(dev,), device_id_type=MESH)
    pl.semaphore_wait(barrier, len(others))

    def part_copy(a, p, rel, d):
        lo, size = PART_ROWS[p]
        return pltpu.make_async_remote_copy(
            src_ref=slots.at[a, SLOT[p, rel], pl.ds(lo, size)],
            dst_ref=slots.at[a, SLOT[p, rel ^ d], pl.ds(lo, size)],
            send_sem=send_sem.at[a, p, SLOT[p, rel ^ d]],
            recv_sem=recv_sem.at[a, p, SLOT[p, rel ^ d]],
            device_id=(peer(d),), device_id_type=MESH)

    def arrival(a, p, rel):
        d = next(x for x in reversed(PART_DIMS[p]) if rel & x)
        part_copy(a, p, rel ^ d, d).wait_recv()

    pair_copies = [pltpu.make_async_remote_copy(
        src_ref=slots.at[a, 0], dst_ref=slots.at[a, 1], send_sem=pair_send.at[a], recv_sem=pair_recv.at[a],
        device_id=(other_core,), device_id_type=MESH) for a in range(2)]
    pair_copies.append(pltpu.make_async_remote_copy(
        src_ref=id_rows.at[pl.ds(0, ROWS)], dst_ref=id_rows.at[pl.ds(ROWS, ROWS)], send_sem=pair_send.at[2],
        recv_sem=pair_recv.at[2], device_id=(other_core,), device_id_type=MESH))
    id_copies = []
    for rel in range(1, 8):
        id_copies.append(pltpu.make_async_remote_copy(
            src_ref=ids_raw.at[0], dst_ref=ids_raw.at[rel], send_sem=ids_send.at[rel],
            recv_sem=ids_recv.at[rel], device_id=(peer(rel),), device_id_type=MESH))
    pair_copies[0].start()
    for send in own_sends(0):
        part_copy(0, *send).start()
    for c in img_loads:
        c.wait()
    for c in id_copies:
        c.start()
    slots[1, 0, 0:TILE_M, :] = unit_rows(g0[:, 0:EMBED], head[...])
    slots[1, 0, TILE_M:ROWS, :] = unit_rows(g1[:, 0:EMBED], head[...])
    acc[...] = jnp.zeros_like(acc)
    sums[...] = jnp.zeros_like(sums)
    for c in pair_copies[1:]:
        c.start()
    for send in own_sends(1):
        part_copy(0, *send).start()

    scale, bias = scal_ref[0], scal_ref[1]
    for c in id_copies:
        c.wait_recv()
    lane = lax.broadcasted_iota(jnp.int32, (1, ROWS), 1)
    ids_all[0] = ids_raw[0]
    for turn in range(7):
        ids_all[2 + turn] = jnp.where(
            lane < PART_ROWS[1][0], ids_raw[turn_rel(turn, 0)],
            jnp.where(lane < PART_ROWS[2][0], ids_raw[turn_rel(turn, 1)], ids_raw[turn_rel(turn, 2)]))
    for c in pair_copies:
        c.wait_recv()

    n_m = 2 * ROWS // TILE_M

    def slot_of(block):
        return block + (block + 7) // 8

    def row_tile(t):
        return (t % n_m + (n_m // 2) * ((t // n_m + 7) // 8)) % n_m

    def scores(a, t, s_ref):
        m, slot = pl.multiple_of(row_tile(t) * TILE_M, TILE_M), slot_of(t // n_m)
        rows = slots[1 - a, m // ROWS, pl.ds(pl.multiple_of(m % ROWS, TILE_M), TILE_M), :]
        s_ref[...] = lax.dot_general(rows, slots[a, slot], CONTRACT_COLS, preferred_element_type=F32)

    def tile_grad(a, t, s_ref, g_ref):
        m, slot = pl.multiple_of(row_tile(t) * TILE_M, TILE_M), slot_of(t // n_m)

        col_ids = ids_all[slot]

        def rows_step(i, carry):
            x0, x1 = carry
            top = pl.multiple_of(i * CHUNK_R, CHUNK_R)
            row_ids = jnp.concatenate([id_rows[pl.ds(pl.multiple_of(m + top, CHUNK_R), CHUNK_R), :]] * 8, axis=1)
            sim = s_ref[pl.ds(top, CHUNK_R), :]
            sign = jnp.where(row_ids == col_ids, -1.0, 1.0)
            margin = sign * (scale * sim + bias)
            e = jnp.exp2(jnp.abs(margin) * (-LOG2E))
            d = 1.0 + e
            r = 1.0 / d
            grad = sign * jnp.where(margin >= 0, r, e * r)
            g_ref[pl.ds(top, CHUNK_R), :] = grad.astype(BF16)
            if a == 0:
                return x0 + jnp.maximum(margin, 0.0), x1 * d + e
            return x0 + grad * sim, x1 + grad

        x1 = jnp.zeros((CHUNK_R, ROWS), F32) if a == 0 else sums[3]
        x0, x1 = lax.fori_loop(0, TILE_M // CHUNK_R, rows_step, (sums[2 * a], x1), unroll=True)
        sums[2 * a] = x0
        sums[2 * a + 1] = sums[1] + jnp.log1p(x1) if a == 0 else x1

    def row_grad(a, t, g_ref):
        m, slot = pl.multiple_of(row_tile(t) * TILE_M, TILE_M), slot_of(t // n_m)
        acc[1 - a, pl.ds(m, TILE_M), :] += jnp.dot(g_ref[...], slots[a, slot], preferred_element_type=F32)

    def run_turn(a, turn):
        for p in range(3):
            arrival(a, p, turn_rel(turn, p))
        if (a, turn) == (0, 0):
            for send in own_sends(2):
                part_copy(0, *send).start()
        for send in turn_sends(turn):
            part_copy(a, *send).start()
        if a == 0 and 3 <= turn <= 5:
            for send in own_sends(turn - 3):
                part_copy(1, *send).start()

    grad_copies = [pltpu.make_async_remote_copy(
        src_ref=acc.at[x, pl.ds(ROWS, ROWS)], dst_ref=partner.at[x], send_sem=grad_send.at[x],
        recv_sem=grad_recv.at[x], device_id=(other_core,), device_id_type=MESH) for x in range(2)]

    def stream(a, after_loop=lambda: None, near_end=lambda: None):
        t0, t_end = 0, 8 * n_m
        scores(a, t0, s0)
        scores(a, t0 + 1, s1)
        tile_grad(a, t0, s0, g0)

        def body(k, carry):
            t = t0 + 2 * k + 1
            for task, todo in actions[a].items():
                @pl.when(t + 1 == task)
                def _():
                    for act in todo:
                        act()
            scores(a, t + 1, s0)
            tile_grad(a, t, s1, g1)
            row_grad(a, t - 1, g0)
            scores(a, t + 2, s1)
            tile_grad(a, t + 1, s0, g0)
            row_grad(a, t, g1)
            return carry

        lax.fori_loop(0, (t_end - t0 - 2) // 2, body, 0)
        grad_copies[1 - a].start()
        after_loop()
        tile_grad(a, t_end - 1, s1, g1)
        row_grad(a, t_end - 2, g0)
        near_end()
        row_grad(a, t_end - 1, g1)

    half_rows = EMBED // 2
    steps = (64, 32, 16)
    bits = [[(chip // PART_DIMS[p][k]) % 2 for k in range(3)] for p in range(3)]
    lows = [[core * half_rows + 128 * p] for p in range(3)]
    for p in range(3):
        for k in range(3):
            lows[p].append(lows[p][-1] + bits[p][k] * steps[k])
    cols = [pl.ds(h * (EMBED // 2), EMBED // 2) for h in range(2)]
    lanes = [(p, h) for h in range(2) for p in range(3)]
    started = []

    def start(make, *args):
        make(*args).start()
        started.append((make, args))

    def rows_at(low, size, base=0):
        return pl.ds(pl.multiple_of(low + base, 16), size)

    def near(p, k):
        return (peer(PART_DIMS[p][k]),)

    def core_copy(x):
        return pltpu.make_async_remote_copy(
            src_ref=acc.at[x, rows_at((1 - core) * half_rows, half_rows, ROWS)], dst_ref=partner.at[x, pl.ds(0, half_rows)],
            send_sem=core_send.at[x], recv_sem=core_recv.at[x], device_id=(other_core,), device_id_type=MESH)

    def scatter_copy(x, k, p, h):
        return pltpu.make_async_remote_copy(
            src_ref=acc.at[x, rows_at(lows[p][k] + (1 - bits[p][k]) * steps[k], steps[k], ROWS), cols[h]],
            dst_ref=partner.at[x, pl.ds(half_rows + 112 * p + (0, 64, 96)[k], steps[k]), cols[h]],
            send_sem=rs_send.at[x, k, p, h], recv_sem=rs_recv.at[x, k, p, h], device_id=near(p, k), device_id_type=MESH)

    def gather_copy(x, k, p, h):
        rows = rows_at(lows[p][k + 1], steps[k])
        return pltpu.make_async_remote_copy(
            src_ref=acc.at[x, rows, cols[h]], dst_ref=acc.at[x, rows, cols[h]], send_sem=ag_send.at[x, k, p, h],
            recv_sem=ag_recv.at[x, k, p, h], device_id=near(p, k), device_id_type=MESH)

    def share(x, k, p, h):
        rows = rows_at(lows[p][3], 16) if k == 3 else rows_at(lows[p][k] + (1 - bits[p][k]) * steps[k], steps[k])
        return pltpu.make_async_remote_copy(
            src_ref=acc.at[x, rows, cols[h]], dst_ref=acc.at[x, rows, cols[h]], send_sem=out_send.at[x, k, p, h],
            recv_sem=out_recv.at[x, k, p, h], device_id=(other_core,), device_id_type=MESH)

    def late_load(x):
        srcs = ((feat_txt, slots.at[0, 5]), (w_txt, slots.at[0, 6, pl.ds(0, EMBED)])) if x == 0 else (
            (feat_img, slots.at[0, 2]), (w_img, slots.at[0, 3, pl.ds(0, EMBED)]))
        return [pltpu.make_async_copy(src, dst, late_sem.at[x, k]) for k, (src, dst) in enumerate(srcs)]

    def begin_load(x, turns):
        for turn in turns:
            for send in turn_sends(turn):
                part_copy(0, *send).wait_send()
        for c in late_load(x):
            c.start()

    def head_partial(x, between=lambda: None):
        for c in late_load(x):
            c.wait()
        feat, weights = (5, 6) if x == 0 else (2, 3)

        def rows_step(i, carry):
            rows = pl.ds(pl.multiple_of(i * 256, 256), 256)
            raw = jnp.dot(slots[0, feat, rows, :], slots[0, weights, 0:EMBED, :], preferred_element_type=F32)
            inv = lax.rsqrt(jnp.sum(raw * raw, axis=1, keepdims=True))
            unit = raw * inv
            grad = scale * ((acc[x, rows, :] + partner[x, rows, :]) * F32(1.0 / (16 * ROWS)))
            slots[0, 4, rows, :] = (inv * (grad - unit * jnp.sum(unit * grad, axis=1, keepdims=True))).astype(BF16)
            return carry

        lax.fori_loop(0, ROWS // 256, rows_step, 0)
        grad_copies[x].wait_send()
        for dev in [other_core] + [peer(d) for d in (1, 2, 4)]:
            pl.semaphore_signal(ready.at[x], inc=1, device_id=(dev,), device_id_type=MESH)
        between()

        def half_grad(which):
            cut = pl.ds(pl.multiple_of(which * half_rows, half_rows), half_rows)
            acc[x, rows_at(which * half_rows, half_rows, ROWS), :] = lax.dot_general(
                slots[0, feat, :, cut], slots[0, 4], CONTRACT_ROWS, preferred_element_type=F32)

        half_grad(1 - core)
        pl.semaphore_wait(ready.at[x], 4)
        start(core_copy, x)
        half_grad(core)

    def step_first(x):
        core_copy(x).wait_recv()
        acc[x, rows_at(core * half_rows, half_rows, ROWS), :] += partner[x, 0:half_rows, :]
        for p, h in lanes:
            start(scatter_copy, x, 0, p, h)

    def step_scatter(x, k):
        for p, h in lanes:
            scatter_copy(x, k, p, h).wait_recv()
            base = half_rows + 112 * p + (0, 64, 96)[k]
            mine = rows_at(lows[p][k + 1], steps[k], ROWS)
            total = acc[x, mine, cols[h]] + partner[x, base:base + steps[k], cols[h]]
            if k < 2:
                acc[x, mine, cols[h]] = total
                start(scatter_copy, x, k + 1, p, h)
            else:
                acc[x, rows_at(lows[p][3], 16), cols[h]] = total
                start(gather_copy, x, 2, p, h)
                start(share, x, 3, p, h)

    def step_gather(x, k):
        for p, h in lanes:
            gather_copy(x, k, p, h).wait_recv()
            if k > 0:
                start(gather_copy, x, k - 1, p, h)
            start(share, x, k, p, h)

    def step_out(x):
        for k in (3, 2, 1, 0):
            for p, h in lanes:
                share(x, k, p, h).wait_recv()
        outs[x].start()

    outs = [pltpu.make_async_copy(acc.at[x, pl.ds(0, EMBED)], ref, load_sem.at[x])
            for x, ref in ((0, dw_txt_ref), (1, dw_img_ref))]
    actions = [{b * n_m: [lambda a=a, b=b: run_turn(a, b - 1)] for b in range(1, 8)} for a in range(2)]
    actions[0][7 * n_m].append(lambda: begin_load(1, (-1, 0, 1)))
    actions[1][n_m].append(lambda: begin_load(0, (3,)))
    actions[1][4 * n_m].append(lambda: (grad_copies[1].wait_recv(), head_partial(1)))
    actions[1][7 * n_m].append(lambda: step_first(1))
    actions[1][7 * n_m + 2] = [lambda: step_scatter(1, 0)]

    stream(0)
    stream(1, after_loop=lambda: step_scatter(1, 1), near_end=lambda: step_scatter(1, 2))
    for x in range(4):
        rows = sums[x, 0:8, :] + sums[x, 8:16, :]
        stats[me, x] = sum(rows[:, v:v + 128] for v in range(0, ROWS, 128))
    stat_copies = [pltpu.make_async_remote_copy(
        src_ref=stats.at[me], dst_ref=stats.at[me], send_sem=st_send.at[k], recv_sem=st_recv.at[k],
        device_id=(dev,), device_id_type=MESH) for k, dev in enumerate(others)]
    for c in stat_copies:
        c.start()
    grad_copies[0].wait_recv()
    step_gather(1, 2)
    head_partial(0, between=lambda: step_gather(1, 1))
    step_first(0)
    step_scatter(0, 0)
    step_gather(1, 0)
    step_scatter(0, 1)
    step_out(1)
    step_scatter(0, 2)
    for c in stat_copies:
        c.wait_recv()
    total = stats[0]
    for dev in range(1, 16):
        total = total + stats[dev]
    tot_ref[...] = jnp.broadcast_to(jnp.sum(jnp.sum(total, axis=1, keepdims=True), axis=2, keepdims=True), (4, 8, 128))
    for k in (2, 1, 0):
        step_gather(0, k)
    step_out(0)
    for c in pair_copies + id_copies + stat_copies:
        c.wait_send()
    for make, args in started:
        make(*args).wait_send()
    for turn in (-1, 0, 1, 3):
        for send in turn_sends(turn):
            part_copy(1, *send).wait_send()
    for c in outs:
        c.wait()


def solution(mesh):
    n_dev = mesh.shape["data"]

    def local_fn(feat_img, feat_txt, w_img, w_txt, log_temp, logit_bias, pair_ids):
        total_rows = feat_img.shape[0] * n_dev
        temp_scale = jnp.exp(log_temp)
        scal = jnp.stack([temp_scale, logit_bias])
        vmem = pl.BlockSpec(memory_space=pltpu.VMEM)
        smem = pl.BlockSpec(memory_space=pltpu.SMEM)
        hbm = pl.BlockSpec(memory_space=pl.ANY)
        dma = pltpu.SemaphoreType.DMA
        dw_img, dw_txt, totals = pl.pallas_call(
            pair_kernel,
            out_shape=[jax.ShapeDtypeStruct((EMBED, EMBED), F32)] * 2 + [jax.ShapeDtypeStruct((4, 8, 128), F32)],
            in_specs=[smem] + [hbm] * 6,
            out_specs=[hbm, hbm, vmem],
            scratch_shapes=[
                pltpu.VMEM((2, 9, ROWS, EMBED), BF16),
                pltpu.VMEM((8, 1, ROWS), jnp.int32), pltpu.VMEM((9, 1, ROWS), jnp.int32),
                pltpu.VMEM((2 * ROWS, 128), jnp.int32),
                pltpu.VMEM((2, 2 * ROWS, EMBED), F32),
                pltpu.VMEM((2, ROWS, EMBED), F32),
                pltpu.VMEM((TILE_M, ROWS), F32), pltpu.VMEM((TILE_M, ROWS), F32),
                pltpu.VMEM((TILE_M, ROWS), BF16), pltpu.VMEM((TILE_M, ROWS), BF16),
                pltpu.VMEM((4, CHUNK_R, ROWS), F32), pltpu.VMEM((16, 4, 8, 128), F32), pltpu.VMEM((EMBED, EMBED), BF16),
                dma((2, 3, 9)), dma((2, 3, 9)), dma((9,)), dma((9,)), dma((3,)), dma((3,)), dma((2,)), dma((2,)),
                dma((7,)), dma((2, 2)), dma((2,)), dma((2,)), dma((2, 3, 3, 2)), dma((2, 3, 3, 2)), dma((2, 3, 3, 2)),
                dma((2, 3, 3, 2)), dma((2, 4, 3, 2)), dma((2, 4, 3, 2)), dma((15,)), dma((15,)),
                pltpu.SemaphoreType.REGULAR((2,)),
            ],
            compiler_params=pltpu.CompilerParams(
                collective_id=0, has_side_effects=True, vmem_limit_bytes=66_000_000),
            cost_estimate=pl.CostEstimate(flops=110_000_000_000, bytes_accessed=16_000_000, transcendentals=0),
        )(scal, feat_img, feat_txt, w_img, w_txt, pair_ids.reshape(1, ROWS),
          jnp.broadcast_to(pair_ids[:, None], (ROWS, 128)))
        loss_sum, temp_sum, bias_sum = totals[0, 0, 0] + totals[1, 0, 0], totals[2, 0, 0], totals[3, 0, 0]
        return loss_sum / total_rows, temp_scale * (temp_sum / total_rows), bias_sum / total_rows, dw_img, dw_txt

    return jax.shard_map(
        local_fn,
        mesh=mesh,
        in_specs=(P("data", None), P("data", None), P(None, None), P(None, None), P(), P(), P("data")),
        out_specs=(P(), P(), P(), P(None, None), P(None, None)),
        check_vma=False,
    )
```

```python
import jax
import jax.numpy as jnp
from jax import lax
from jax.experimental import pallas as pl
from jax.experimental.pallas import tpu as pltpu
from jax.sharding import PartitionSpec as P

F32, BF16 = jnp.float32, jnp.bfloat16
MESH = pl.DeviceIdType.MESH
ROWS, EMBED = 1024, 768
TILE_M, CHUNK_R = 512, 16
LOG2E = 1.4426950408889634
CONTRACT_ROWS = (((0,), (0,)), ((), ()))
CONTRACT_COLS = (((1,), (1,)), ((), ()))

PART_ROWS = ((0, 352), (352, 336), (688, 336))
PART_DIMS = ((1, 2, 4), (2, 4, 1), (4, 1, 2))


def turn_rel(turn, part):
    dims = PART_DIMS[part]
    return {0: dims[0], 1: dims[1], 2: dims[2], 3: dims[0] | dims[1], 4: dims[0] | dims[2], 5: dims[1] | dims[2],
            6: 7}[turn]


SLOT = {(part, turn_rel(turn, part)): 2 + turn for turn in range(7) for part in range(3)}
SLOT.update({(part, 0): 0 for part in range(3)})


def own_sends(k):
    return [(p, 0, PART_DIMS[p][k]) for p in range(3)]


def turn_sends(turn):
    ways = {-1: ((None, 0), (None, 1), (None, 2)), 0: ((0, 1), (0, 2)), 1: ((1, 2),), 3: ((3, 2),)}.get(turn, ())
    return [(p, 0 if turn < 0 else turn_rel(turn, p), PART_DIMS[p][k]) for _, k in ways for p in range(3)]


def pair_kernel(scal_ref, feat_img, feat_txt, w_img, w_txt, ids_ref, dw_img_ref, dw_txt_ref, tot_ref,
                slots, ids_raw, ids_all, id_rows, acc, partner, s0, s1, g0, g1, sums, stats, head,
                send_sem, recv_sem, ids_send, ids_recv, pair_send, pair_recv, grad_send, grad_recv, load_sem,
                late_sem, core_send, core_recv, rs_send, rs_recv, ag_send, ag_recv, out_send, out_recv, st_send, st_recv, ready):
    me = lax.axis_index("data")
    core = me % 2
    chip = me // 2

    def peer(rel):
        where = chip
        for d in (1, 2, 4):
            if rel & d:
                where = where + d * (1 - 2 * ((chip // d) % 2))
        return where * 2 + core

    other_core = chip * 2 + (1 - core)
    txt_loads = [pltpu.make_async_copy(feat_txt, slots.at[0, 8], load_sem.at[0]),
                 pltpu.make_async_copy(w_txt, slots.at[0, 7, pl.ds(0, EMBED)], load_sem.at[1])]
    img_loads = [pltpu.make_async_copy(feat_img.at[pl.ds(0, TILE_M)], g0.at[:, pl.ds(0, EMBED)], load_sem.at[2]),
                 pltpu.make_async_copy(feat_img.at[pl.ds(TILE_M, TILE_M)], g1.at[:, pl.ds(0, EMBED)], load_sem.at[3]),
                 pltpu.make_async_copy(w_img, head, load_sem.at[4]),
                 pltpu.make_async_copy(ids_ref, ids_raw.at[0], load_sem.at[5])]
    for c in txt_loads + img_loads:
        c.start()
    for c in txt_loads:
        c.wait()

    def unit_rows(feat_rows, weights):
        raw = jnp.dot(feat_rows, weights, preferred_element_type=F32)
        return (raw * lax.rsqrt(jnp.sum(raw * raw, axis=1, keepdims=True))).astype(BF16)

    def embed_txt(i, carry):
        rows = pl.ds(pl.multiple_of(i * TILE_M, TILE_M), TILE_M)
        slots[0, 0, rows, :] = unit_rows(slots[0, 8, rows, :], slots[0, 7, 0:EMBED, :])
        return carry

    lax.fori_loop(0, ROWS // TILE_M, embed_txt, 0)

    barrier = pltpu.get_barrier_semaphore()
    others = [(me + k) % 16 for k in range(1, 16)]
    for dev in others:
        pl.semaphore_signal(barrier, inc=1, device_id=(dev,), device_id_type=MESH)
    pl.semaphore_wait(barrier, len(others))

    def part_copy(a, p, rel, d):
        lo, size = PART_ROWS[p]
        return pltpu.make_async_remote_copy(
            src_ref=slots.at[a, SLOT[p, rel], pl.ds(lo, size)],
            dst_ref=slots.at[a, SLOT[p, rel ^ d], pl.ds(lo, size)],
            send_sem=send_sem.at[a, p, SLOT[p, rel ^ d]],
            recv_sem=recv_sem.at[a, p, SLOT[p, rel ^ d]],
            device_id=(peer(d),), device_id_type=MESH)

    def arrival(a, p, rel):
        d = next(x for x in reversed(PART_DIMS[p]) if rel & x)
        part_copy(a, p, rel ^ d, d).wait_recv()

    pair_copies = [pltpu.make_async_remote_copy(
        src_ref=slots.at[a, 0], dst_ref=slots.at[a, 1], send_sem=pair_send.at[a], recv_sem=pair_recv.at[a],
        device_id=(other_core,), device_id_type=MESH) for a in range(2)]
    pair_copies.append(pltpu.make_async_remote_copy(
        src_ref=id_rows.at[pl.ds(0, ROWS)], dst_ref=id_rows.at[pl.ds(ROWS, ROWS)], send_sem=pair_send.at[2],
        recv_sem=pair_recv.at[2], device_id=(other_core,), device_id_type=MESH))
    id_copies = []
    for rel in range(1, 8):
        id_copies.append(pltpu.make_async_remote_copy(
            src_ref=ids_raw.at[0], dst_ref=ids_raw.at[rel], send_sem=ids_send.at[rel],
            recv_sem=ids_recv.at[rel], device_id=(peer(rel),), device_id_type=MESH))
    pair_copies[0].start()
    for send in own_sends(0):
        part_copy(0, *send).start()
    for c in img_loads:
        c.wait()
    for c in id_copies:
        c.start()
    for k in range(0, ROWS, 128):
        id_rows[k:k + 128, :] = jnp.broadcast_to(ids_raw[0, :, k:k + 128], (128, 128)).T
    slots[1, 0, 0:TILE_M, :] = unit_rows(g0[:, 0:EMBED], head[...])
    slots[1, 0, TILE_M:ROWS, :] = unit_rows(g1[:, 0:EMBED], head[...])
    acc[...] = jnp.zeros_like(acc)
    sums[...] = jnp.zeros_like(sums)
    for c in pair_copies[1:]:
        c.start()
    for send in own_sends(1):
        part_copy(0, *send).start()

    scale, bias = scal_ref[0], scal_ref[1]
    for c in id_copies:
        c.wait_recv()
    lane = lax.broadcasted_iota(jnp.int32, (1, ROWS), 1)
    ids_all[0] = ids_raw[0]
    for turn in range(7):
        ids_all[2 + turn] = jnp.where(
            lane < PART_ROWS[1][0], ids_raw[turn_rel(turn, 0)],
            jnp.where(lane < PART_ROWS[2][0], ids_raw[turn_rel(turn, 1)], ids_raw[turn_rel(turn, 2)]))
    for c in pair_copies:
        c.wait_recv()

    n_m = 2 * ROWS // TILE_M

    def slot_of(block):
        return block + (block + 7) // 8

    def row_tile(t):
        return (t % n_m + (n_m // 2) * ((t // n_m + 7) // 8)) % n_m

    def scores(a, t, s_ref):
        m, slot = pl.multiple_of(row_tile(t) * TILE_M, TILE_M), slot_of(t // n_m)
        rows = slots[1 - a, m // ROWS, pl.ds(pl.multiple_of(m % ROWS, TILE_M), TILE_M), :]
        s_ref[...] = lax.dot_general(rows, slots[a, slot], CONTRACT_COLS, preferred_element_type=F32)

    def tile_grad(a, t, s_ref, g_ref):
        m, slot = pl.multiple_of(row_tile(t) * TILE_M, TILE_M), slot_of(t // n_m)

        col_ids = ids_all[slot]

        def rows_step(i, carry):
            x0, x1 = carry
            top = pl.multiple_of(i * CHUNK_R, CHUNK_R)
            row_ids = jnp.concatenate([id_rows[pl.ds(pl.multiple_of(m + top, CHUNK_R), CHUNK_R), :]] * 8, axis=1)
            sim = s_ref[pl.ds(top, CHUNK_R), :]
            sign = jnp.where(row_ids == col_ids, -1.0, 1.0)
            margin = sign * (scale * sim + bias)
            e = jnp.exp2(jnp.abs(margin) * (-LOG2E))
            d = 1.0 + e
            r = 1.0 / d
            grad = sign * jnp.where(margin >= 0, r, e * r)
            g_ref[pl.ds(top, CHUNK_R), :] = grad.astype(BF16)
            if a == 0:
                return x0 + jnp.maximum(margin, 0.0), x1 * d + e
            return x0 + grad * sim, x1 + grad

        x1 = jnp.zeros((CHUNK_R, ROWS), F32) if a == 0 else sums[3]
        x0, x1 = lax.fori_loop(0, TILE_M // CHUNK_R, rows_step, (sums[2 * a], x1), unroll=True)
        sums[2 * a] = x0
        sums[2 * a + 1] = sums[1] + jnp.log1p(x1) if a == 0 else x1

    def row_grad(a, t, g_ref):
        m, slot = pl.multiple_of(row_tile(t) * TILE_M, TILE_M), slot_of(t // n_m)
        acc[1 - a, pl.ds(m, TILE_M), :] += jnp.dot(g_ref[...], slots[a, slot], preferred_element_type=F32)

    def run_turn(a, turn):
        for p in range(3):
            arrival(a, p, turn_rel(turn, p))
        if (a, turn) == (0, 0):
            for send in own_sends(2):
                part_copy(0, *send).start()
        for send in turn_sends(turn):
            part_copy(a, *send).start()
        if a == 0 and 3 <= turn <= 5:
            for send in own_sends(turn - 3):
                part_copy(1, *send).start()

    grad_copies = [pltpu.make_async_remote_copy(
        src_ref=acc.at[x, pl.ds(ROWS, ROWS)], dst_ref=partner.at[x], send_sem=grad_send.at[x],
        recv_sem=grad_recv.at[x], device_id=(other_core,), device_id_type=MESH) for x in range(2)]

    def stream(a, after_loop=lambda: None, near_end=lambda: None):
        t0, t_end = 0, 8 * n_m
        scores(a, t0, s0)
        scores(a, t0 + 1, s1)
        tile_grad(a, t0, s0, g0)

        def body(k, carry):
            t = t0 + 2 * k + 1
            for task, todo in actions[a].items():
                @pl.when(t + 1 == task)
                def _():
                    for act in todo:
                        act()
            scores(a, t + 1, s0)
            tile_grad(a, t, s1, g1)
            row_grad(a, t - 1, g0)
            scores(a, t + 2, s1)
            tile_grad(a, t + 1, s0, g0)
            row_grad(a, t, g1)
            return carry

        lax.fori_loop(0, (t_end - t0 - 2) // 2, body, 0)
        grad_copies[1 - a].start()
        after_loop()
        tile_grad(a, t_end - 1, s1, g1)
        row_grad(a, t_end - 2, g0)
        near_end()
        row_grad(a, t_end - 1, g1)

    half_rows = EMBED // 2
    steps = (64, 32, 16)
    bits = [[(chip // PART_DIMS[p][k]) % 2 for k in range(3)] for p in range(3)]
    lows = [[core * half_rows + 128 * p] for p in range(3)]
    for p in range(3):
        for k in range(3):
            lows[p].append(lows[p][-1] + bits[p][k] * steps[k])
    cols = [pl.ds(h * (EMBED // 2), EMBED // 2) for h in range(2)]
    lanes = [(p, h) for h in range(2) for p in range(3)]
    started = []

    def start(make, *args):
        make(*args).start()
        started.append((make, args))

    def rows_at(low, size, base=0):
        return pl.ds(pl.multiple_of(low + base, 16), size)

    def near(p, k):
        return (peer(PART_DIMS[p][k]),)

    def core_copy(x):
        return pltpu.make_async_remote_copy(
            src_ref=acc.at[x, rows_at((1 - core) * half_rows, half_rows, ROWS)], dst_ref=partner.at[x, pl.ds(0, half_rows)],
            send_sem=core_send.at[x], recv_sem=core_recv.at[x], device_id=(other_core,), device_id_type=MESH)

    def scatter_copy(x, k, p, h):
        return pltpu.make_async_remote_copy(
            src_ref=acc.at[x, rows_at(lows[p][k] + (1 - bits[p][k]) * steps[k], steps[k], ROWS), cols[h]],
            dst_ref=partner.at[x, pl.ds(half_rows + 112 * p + (0, 64, 96)[k], steps[k]), cols[h]],
            send_sem=rs_send.at[x, k, p, h], recv_sem=rs_recv.at[x, k, p, h], device_id=near(p, k), device_id_type=MESH)

    def gather_copy(x, k, p, h):
        rows = rows_at(lows[p][k + 1], steps[k])
        return pltpu.make_async_remote_copy(
            src_ref=acc.at[x, rows, cols[h]], dst_ref=acc.at[x, rows, cols[h]], send_sem=ag_send.at[x, k, p, h],
            recv_sem=ag_recv.at[x, k, p, h], device_id=near(p, k), device_id_type=MESH)

    def share(x, k, p, h):
        rows = rows_at(lows[p][3], 16) if k == 3 else rows_at(lows[p][k] + (1 - bits[p][k]) * steps[k], steps[k])
        return pltpu.make_async_remote_copy(
            src_ref=acc.at[x, rows, cols[h]], dst_ref=acc.at[x, rows, cols[h]], send_sem=out_send.at[x, k, p, h],
            recv_sem=out_recv.at[x, k, p, h], device_id=(other_core,), device_id_type=MESH)

    def late_load(x):
        srcs = ((feat_txt, slots.at[0, 5]), (w_txt, slots.at[0, 6, pl.ds(0, EMBED)])) if x == 0 else (
            (feat_img, slots.at[0, 2]), (w_img, slots.at[0, 3, pl.ds(0, EMBED)]))
        return [pltpu.make_async_copy(src, dst, late_sem.at[x, k]) for k, (src, dst) in enumerate(srcs)]

    def begin_load(x, turns):
        for turn in turns:
            for send in turn_sends(turn):
                part_copy(0, *send).wait_send()
        for c in late_load(x):
            c.start()

    def head_partial(x, between=lambda: None):
        for c in late_load(x):
            c.wait()
        feat, weights = (5, 6) if x == 0 else (2, 3)

        def rows_step(i, carry):
            rows = pl.ds(pl.multiple_of(i * 256, 256), 256)
            raw = jnp.dot(slots[0, feat, rows, :], slots[0, weights, 0:EMBED, :], preferred_element_type=F32)
            inv = lax.rsqrt(jnp.sum(raw * raw, axis=1, keepdims=True))
            unit = raw * inv
            grad = scale * ((acc[x, rows, :] + partner[x, rows, :]) * F32(1.0 / (16 * ROWS)))
            slots[0, 4, rows, :] = (inv * (grad - unit * jnp.sum(unit * grad, axis=1, keepdims=True))).astype(BF16)
            return carry

        lax.fori_loop(0, ROWS // 256, rows_step, 0)
        grad_copies[x].wait_send()
        for dev in [other_core] + [peer(d) for d in (1, 2, 4)]:
            pl.semaphore_signal(ready.at[x], inc=1, device_id=(dev,), device_id_type=MESH)
        between()

        def half_grad(which):
            cut = pl.ds(pl.multiple_of(which * half_rows, half_rows), half_rows)
            acc[x, rows_at(which * half_rows, half_rows, ROWS), :] = lax.dot_general(
                slots[0, feat, :, cut], slots[0, 4], CONTRACT_ROWS, preferred_element_type=F32)

        half_grad(1 - core)
        pl.semaphore_wait(ready.at[x], 4)
        start(core_copy, x)
        half_grad(core)

    def step_first(x):
        core_copy(x).wait_recv()
        acc[x, rows_at(core * half_rows, half_rows, ROWS), :] += partner[x, 0:half_rows, :]
        for p, h in lanes:
            start(scatter_copy, x, 0, p, h)

    def step_scatter(x, k):
        for p, h in lanes:
            scatter_copy(x, k, p, h).wait_recv()
            base = half_rows + 112 * p + (0, 64, 96)[k]
            mine = rows_at(lows[p][k + 1], steps[k], ROWS)
            total = acc[x, mine, cols[h]] + partner[x, base:base + steps[k], cols[h]]
            if k < 2:
                acc[x, mine, cols[h]] = total
                start(scatter_copy, x, k + 1, p, h)
            else:
                acc[x, rows_at(lows[p][3], 16), cols[h]] = total
                start(gather_copy, x, 2, p, h)
                start(share, x, 3, p, h)

    def step_gather(x, k):
        for p, h in lanes:
            gather_copy(x, k, p, h).wait_recv()
            if k > 0:
                start(gather_copy, x, k - 1, p, h)
            start(share, x, k, p, h)

    def step_out(x):
        for k in (3, 2, 1, 0):
            for p, h in lanes:
                share(x, k, p, h).wait_recv()
        outs[x].start()

    outs = [pltpu.make_async_copy(acc.at[x, pl.ds(0, EMBED)], ref, load_sem.at[x])
            for x, ref in ((0, dw_txt_ref), (1, dw_img_ref))]
    actions = [{b * n_m: [lambda a=a, b=b: run_turn(a, b - 1)] for b in range(1, 8)} for a in range(2)]
    actions[0][7 * n_m].append(lambda: begin_load(1, (-1, 0, 1)))
    actions[1][n_m].append(lambda: begin_load(0, (3,)))
    actions[1][4 * n_m].append(lambda: (grad_copies[1].wait_recv(), head_partial(1)))
    actions[1][7 * n_m].append(lambda: step_first(1))
    actions[1][7 * n_m + 2] = [lambda: step_scatter(1, 0)]

    stream(0)
    stream(1, after_loop=lambda: step_scatter(1, 1), near_end=lambda: step_scatter(1, 2))
    for x in range(4):
        rows = sums[x, 0:8, :] + sums[x, 8:16, :]
        stats[me, x] = sum(rows[:, v:v + 128] for v in range(0, ROWS, 128))
    stat_copies = [pltpu.make_async_remote_copy(
        src_ref=stats.at[me], dst_ref=stats.at[me], send_sem=st_send.at[k], recv_sem=st_recv.at[k],
        device_id=(dev,), device_id_type=MESH) for k, dev in enumerate(others)]
    for c in stat_copies:
        c.start()
    grad_copies[0].wait_recv()
    step_gather(1, 2)
    head_partial(0, between=lambda: step_gather(1, 1))
    step_first(0)
    step_scatter(0, 0)
    step_gather(1, 0)
    step_scatter(0, 1)
    step_out(1)
    step_scatter(0, 2)
    for c in stat_copies:
        c.wait_recv()
    total = stats[0]
    for dev in range(1, 16):
        total = total + stats[dev]
    tot_ref[...] = jnp.broadcast_to(jnp.sum(jnp.sum(total, axis=1, keepdims=True), axis=2, keepdims=True), (4, 8, 128))
    for k in (2, 1, 0):
        step_gather(0, k)
    step_out(0)
    for c in pair_copies + id_copies + stat_copies:
        c.wait_send()
    for make, args in started:
        make(*args).wait_send()
    for turn in (-1, 0, 1, 3):
        for send in turn_sends(turn):
            part_copy(1, *send).wait_send()
    for c in outs:
        c.wait()


def solution(mesh):
    n_dev = mesh.shape["data"]

    def local_fn(feat_img, feat_txt, w_img, w_txt, log_temp, logit_bias, pair_ids):
        total_rows = feat_img.shape[0] * n_dev
        temp_scale = jnp.exp(log_temp)
        scal = jnp.stack([temp_scale, logit_bias])
        vmem = pl.BlockSpec(memory_space=pltpu.VMEM)
        smem = pl.BlockSpec(memory_space=pltpu.SMEM)
        hbm = pl.BlockSpec(memory_space=pl.ANY)
        dma = pltpu.SemaphoreType.DMA
        dw_img, dw_txt, totals = pl.pallas_call(
            pair_kernel,
            out_shape=[jax.ShapeDtypeStruct((EMBED, EMBED), F32)] * 2 + [jax.ShapeDtypeStruct((4, 8, 128), F32)],
            in_specs=[smem] + [hbm] * 5,
            out_specs=[hbm, hbm, vmem],
            scratch_shapes=[
                pltpu.VMEM((2, 9, ROWS, EMBED), BF16),
                pltpu.VMEM((8, 1, ROWS), jnp.int32), pltpu.VMEM((9, 1, ROWS), jnp.int32),
                pltpu.VMEM((2 * ROWS, 128), jnp.int32),
                pltpu.VMEM((2, 2 * ROWS, EMBED), F32),
                pltpu.VMEM((2, ROWS, EMBED), F32),
                pltpu.VMEM((TILE_M, ROWS), F32), pltpu.VMEM((TILE_M, ROWS), F32),
                pltpu.VMEM((TILE_M, ROWS), BF16), pltpu.VMEM((TILE_M, ROWS), BF16),
                pltpu.VMEM((4, CHUNK_R, ROWS), F32), pltpu.VMEM((16, 4, 8, 128), F32), pltpu.VMEM((EMBED, EMBED), BF16),
                dma((2, 3, 9)), dma((2, 3, 9)), dma((9,)), dma((9,)), dma((3,)), dma((3,)), dma((2,)), dma((2,)),
                dma((7,)), dma((2, 2)), dma((2,)), dma((2,)), dma((2, 3, 3, 2)), dma((2, 3, 3, 2)), dma((2, 3, 3, 2)),
                dma((2, 3, 3, 2)), dma((2, 4, 3, 2)), dma((2, 4, 3, 2)), dma((15,)), dma((15,)),
                pltpu.SemaphoreType.REGULAR((2,)),
            ],
            compiler_params=pltpu.CompilerParams(
                collective_id=0, has_side_effects=True, vmem_limit_bytes=66_000_000),
            cost_estimate=pl.CostEstimate(flops=110_000_000_000, bytes_accessed=16_000_000, transcendentals=0),
        )(scal, feat_img, feat_txt, w_img, w_txt, pair_ids.reshape(1, ROWS))
        loss_sum, temp_sum, bias_sum = totals[0, 0, 0] + totals[1, 0, 0], totals[2, 0, 0], totals[3, 0, 0]
        return loss_sum / total_rows, temp_scale * (temp_sum / total_rows), bias_sum / total_rows, dw_img, dw_txt

    return jax.shard_map(
        local_fn,
        mesh=mesh,
        in_specs=(P("data", None), P("data", None), P(None, None), P(None, None), P(), P(), P("data")),
        out_specs=(P(), P(), P(), P(None, None), P(None, None)),
        check_vma=False,
    )
```
